8 devices in a mesh: tp: 8 (over z, y, x, core).
Axes of the slice: x: 2, y: 2, z: 1, core: 2. Of those that a mesh axis runs over, the one named last changes fastest.
Arguments:
- x_norm: bfloat16 [8192, 1024], P(None, 'tp')
- hid_act: bfloat16 [8192, 2816], P(None, 'tp')
- dy_in: bfloat16 [2, 8192, 2816], replicated
- dy_out: bfloat16 [8192, 1024], replicated
- w_in: float32 [2, 1024, 2816], P(None, 'tp')
- w_out: float32 [2816, 1024], P('tp')
- row_in: float32 [2, 1024], P(None, 'tp')
- col_in: float32 [2, 2816], replicated
- row_out: float32 [2816], P('tp')
- col_out: float32 [1024], replicated
- beta_two: float32 [], replicated
- rel_step: float32 [], replicated
- clip_rms: float32 [], replicated
- clip_norm: float32 [], replicated
Outputs:
- output 1: float32 [2, 1024, 2816], P(None, 'tp')
- output 2: float32 [2, 1024], P(None, 'tp')
- output 3: float32 [2, 2816], replicated
- output 4: float32 [2816, 1024], P('tp')
- output 5: float32 [2816], P('tp')
- output 6: float32 [1024], replicated
All inputs are finite; a program needn't handle non-finite values.
Results may differ from the reference program's by a relative error of at most 0.001.
Values are sent between devices in bfloat16 or wider.
A program may use at most 1 GiB of HBM per device.

```python
import jax
import jax.numpy as jnp
from jax import lax

D = 1024
FF = 2816
TOK_DEV = 1024
GROUP = 8
TOKENS = TOK_DEV * GROUP
EPS_ONE = 1e-30
EPS_TWO = 1e-3


def setup_inputs(seed: int = 0) -> dict:
    key_list = jax.random.split(jax.random.key(seed), 14)
    x_norm = jax.random.normal(key_list[0], (TOKENS, D), jnp.float32).astype(jnp.bfloat16)
    hid_act = jax.random.normal(key_list[1], (TOKENS, FF), jnp.float32).astype(jnp.bfloat16)
    dy_in = jax.random.normal(key_list[2], (2, TOKENS, FF), jnp.float32).astype(jnp.bfloat16)
    dy_out = jax.random.normal(key_list[3], (TOKENS, D), jnp.float32).astype(jnp.bfloat16)
    w_in = jax.random.normal(key_list[4], (2, D, FF), jnp.float32) * (D ** -0.5)
    w_out = jax.random.normal(key_list[5], (FF, D), jnp.float32) * (FF ** -0.5)
    stat_level = 0.2 * TOKENS
    row_in = stat_level * jax.random.uniform(key_list[6], (2, D), jnp.float32, minval=0.3, maxval=1.7)
    col_in = stat_level * jax.random.uniform(key_list[7], (2, FF), jnp.float32, minval=0.3, maxval=1.7)
    row_out = stat_level * jax.random.uniform(key_list[8], (FF,), jnp.float32, minval=0.3, maxval=1.7)
    col_out = stat_level * jax.random.uniform(key_list[9], (D,), jnp.float32, minval=0.3, maxval=1.7)
    beta_two = jax.random.uniform(key_list[10], (), jnp.float32, minval=0.5, maxval=0.9)
    rel_step = jax.random.uniform(key_list[11], (), jnp.float32, minval=0.2, maxval=0.8)
    clip_rms = jax.random.uniform(key_list[12], (), jnp.float32, minval=0.2, maxval=0.4)
    clip_frac = jax.random.uniform(key_list[13], (), jnp.float32, minval=0.35, maxval=0.6)
    clip_norm = clip_frac * (3.0 * TOKENS * D * FF) ** 0.5
    return {"x_norm": x_norm, "hid_act": hid_act, "dy_in": dy_in, "dy_out": dy_out,
            "w_in": w_in, "w_out": w_out, "row_in": row_in, "col_in": col_in,
            "row_out": row_out, "col_out": col_out, "beta_two": beta_two,
            "rel_step": rel_step, "clip_rms": clip_rms, "clip_norm": clip_norm}


def adafactor_update(weight, gradient, row_stat, col_stat, beta_two, rel_step, clip_rms, grad_scale):
    scaled = grad_scale * gradient
    sq_grad = scaled * scaled + EPS_ONE
    mix_new = 1.0 - beta_two
    row_new = beta_two * row_stat + mix_new * jnp.mean(sq_grad, axis=-1)
    col_new = beta_two * col_stat + mix_new * jnp.mean(sq_grad, axis=-2)
    row_level = jnp.mean(row_new, axis=-1, keepdims=True)
    second = (row_new / row_level)[..., :, None] * col_new[..., None, :]
    update = scaled / jnp.sqrt(second)
    upd_rms = jnp.sqrt(jnp.mean(update * update, axis=(-2, -1), keepdims=True))
    clipped = update / jnp.maximum(1.0, upd_rms / clip_rms)
    w_rms = jnp.sqrt(jnp.mean(weight * weight, axis=(-2, -1), keepdims=True))
    step_size = rel_step * jnp.maximum(EPS_TWO, w_rms)
    return weight - step_size * clipped, row_new, col_new


def reference(x_norm, hid_act, dy_in, dy_out, w_in, w_out, row_in, col_in, row_out, col_out, beta_two, rel_step, clip_rms, clip_norm):
    def input_grad(dy_one):
        return jnp.dot(x_norm.T, dy_one, preferred_element_type=jnp.float32)
    grad_in = lax.map(input_grad, dy_in)
    grad_out = jnp.dot(hid_act.T, dy_out, preferred_element_type=jnp.float32)
    norm_sq = jnp.sum(grad_in * grad_in) + jnp.sum(grad_out * grad_out)
    grad_scale = jnp.minimum(1.0, clip_norm / jnp.sqrt(norm_sq))
    new_in = adafactor_update(w_in, grad_in, row_in, col_in, beta_two, rel_step, clip_rms, grad_scale)
    new_out = adafactor_update(w_out, grad_out, row_out, col_out, beta_two, rel_step, clip_rms, grad_scale)
    return (new_in[0], new_in[1], new_in[2], new_out[0], new_out[1], new_out[2])
```

```python
import jax
import jax.numpy as jnp
from jax import lax
from jax.experimental import pallas as pl
from jax.experimental.pallas import tpu as pltpu
from jax.sharding import PartitionSpec as P

EPS_ONE = 1e-30
EPS_TWO = 1e-3
MESH = pl.DeviceIdType.MESH
F32 = jnp.float32

T = 8192
D = 1024
FF = 2816
ND = 8
XR = D // ND
HR = FF // ND
KC = 1024
NC = T // KC
NB_IN = FF // 128
NB_OUT = D // 128
ROWS_OUT = ((0, 128), (128, 128), (256, HR - 256))


def total(v):
    return jnp.sum(jnp.sum(v, axis=0, keepdims=True), axis=1, keepdims=True)


def spread(row):
    return jnp.broadcast_to(row, (128, row.shape[1])).T


def unspread(col):
    return jnp.broadcast_to(col, (128, 128)).T[0:1, :]


def grad_kernel(x_hbm, hid_hbm, dyi_hbm, dyo_hbm, wi_hbm, wo_hbm, ri_hbm, ci_hbm, ro_hbm, co_hbm,
                beta_hbm, rel_hbm, crms_hbm, cnorm_hbm,
                d_in, d_out, w_in, w_out, rin_new, cin_new, rout_new, cout_new, kappa,
                x_own, x_peer, xt, hid, ring, acc, grecv, m1, m2, m3, row_sq, rpad,
                ri, ci, ro, co, beta, rel, crms, cnorm,
                s_x, s_hid, s_dyo, s_dyi, s_w, s_small, xs_send, xs_recv, g_send, g_recv,
                m1_send, m1_recv, m2_send, m2_recv, m3_send, m3_recv):
    me = lax.axis_index("tp")
    core = lax.rem(me, 2)
    other = 1 - core
    peer = me + 1 - 2 * core

    def hid_copy(q):
        c = pl.ds(pl.multiple_of(q * KC, KC), KC)
        return pltpu.make_async_copy(hid_hbm.at[:, c], hid.at[:, c], s_hid.at[q])

    def dyo_copy(q, slot, half):
        return pltpu.make_async_copy(dyo_hbm.at[pl.ds(pl.multiple_of(q * KC, KC), KC), :],
                                     ring.at[slot, :, pl.ds(half * D, D)], s_dyo.at[q])

    def dyi_copy(i):
        return pltpu.make_async_copy(dyi_hbm.at[core, pl.ds(pl.multiple_of(i * KC, KC), KC), :],
                                     ring.at[lax.rem(i, 3)], s_dyi.at[lax.rem(i, 3)])

    def x_send(i):
        c = pl.ds(pl.multiple_of(i * KC, KC), KC)
        return pltpu.make_async_remote_copy(x_own.at[c, :], x_peer.at[c, :], xs_send.at[i], xs_recv.at[i],
                                            device_id=(peer,), device_id_type=MESH)

    def bcast(buf, send, recv):
        return [pltpu.make_async_remote_copy(buf.at[me], buf.at[me], send.at[k], recv.at[me],
                                             device_id=(lax.rem(me + k, ND),), device_id_type=MESH)
                for k in range(1, ND)]

    def arrivals(buf, send, recv):
        out = []
        for k in range(1, ND):
            src = lax.rem(me + k, ND)
            out.append(pltpu.make_async_remote_copy(buf.at[src], buf.at[src], send.at[k], recv.at[src],
                                                    device_id=(src,), device_id_type=MESH))
        return out

    def exchange_wait(buf, send, recv):
        for cp in arrivals(buf, send, recv):
            cp.wait_recv()

    x_load = pltpu.make_async_copy(x_hbm, x_own, s_x)
    x_load.start()
    hid_copy(0).start()
    dyo_copy(0, 2, 0).start()
    hid_copy(1).start()
    dyo_copy(1, 2, 1).start()
    dyi_copy(0).start()
    small = [pltpu.make_async_copy(a, b, s_small.at[n]) for n, (a, b) in enumerate(
        ((ri_hbm, ri), (ci_hbm, ci), (ro_hbm, ro), (co_hbm, co),
         (beta_hbm, beta), (rel_hbm, rel), (crms_hbm, crms), (cnorm_hbm, cnorm)))]
    for cp in small:
        cp.start()

    barrier = pltpu.get_barrier_semaphore()
    for k in range(1, ND):
        pl.semaphore_signal(barrier, inc=1, device_id=(lax.rem(me + k, ND),), device_id_type=MESH)
    acc[...] = jnp.zeros_like(acc)
    d_out[...] = jnp.zeros_like(d_out)
    m1[me, NB_IN:24, :] = jnp.zeros((24 - NB_IN, 128), F32)
    m2[me, 8:16, :] = jnp.zeros((8, 128), F32)
    rpad[...] = jnp.zeros_like(rpad)
    pl.semaphore_wait(barrier, ND - 1)

    x_load.wait()
    for i in range(NC):
        x_send(i).start()

    def out_step(q, slot, half):
        hid_copy(q).wait()
        dyo_copy(q, slot, half).wait()
        lhs = hid[:, pl.ds(q * KC, KC)]
        for n in range(D // 256):
            c = pl.ds(n * 256, 256)
            d_out[:, c] += jnp.dot(lhs, ring[slot, :, pl.ds(half * D + n * 256, 256)], preferred_element_type=F32)

    out_step(0, 2, 0)
    dyi_copy(1).start()
    out_step(1, 2, 1)
    dyi_copy(2).start()

    @pl.loop(0, NC)
    def _(i):
        slot = lax.rem(i, 3)
        rows = pl.ds(pl.multiple_of(i * KC, KC), KC)
        x_send(i).wait_recv()
        xt[0:XR, :] = x_own[rows, :].T
        xt[XR:2 * XR, :] = x_peer[rows, :].T
        dyi_copy(i).wait()
        for n in range(FF // 256):
            c = pl.ds(n * 256, 256)
            acc[:, c] += jnp.dot(xt[...], ring[slot, :, c], preferred_element_type=F32)

        @pl.when(i < NC - 3)
        def _():
            dyi_copy(i + 3).start()

        @pl.when(i >= NC - 3)
        def _():
            q = 2 * (i - (NC - 4))
            hid_copy(q).start()
            dyo_copy(q, slot, 0).start()
            hid_copy(q + 1).start()
            dyo_copy(q + 1, slot, 1).start()

    loads = [pltpu.make_async_copy(wi_hbm, w_in, s_w.at[0]), pltpu.make_async_copy(wo_hbm, w_out, s_w.at[1])]
    for cp in loads:
        cp.start()

    for j in range(NB_IN):
        g = acc[:, j * 128:(j + 1) * 128]
        m1[me, j:j + 1, :] = jnp.sum(g * g, axis=0, keepdims=True)
    g_copy = pltpu.make_async_remote_copy(acc.at[pl.ds(XR, XR), :], grecv, g_send, g_recv,
                                          device_id=(peer,), device_id_type=MESH)
    g_copy.start()
    m1_out = bcast(m1, m1_send, m1_recv)
    for cp in m1_out:
        cp.start()

    out_step(2, 2, 0)
    out_step(3, 2, 1)

    for cp in small:
        cp.wait()
    for cp in loads:
        cp.wait()
    for k in range(2):
        m2[me, 8 + k:9 + k, :] = ri[k:k + 1, :]
        w_sq = jnp.zeros((8, 128), F32)
        for j in range(NB_IN):
            w = w_in[k, :, j * 128:(j + 1) * 128]
            w_sq = w_sq + jnp.sum((w * w).reshape(XR // 8, 8, 128), axis=0)
        m2[me, 11 + k:12 + k, :] = jnp.sum(w_sq, axis=0, keepdims=True)
    rpad[:, 0:HR] = ro[...].reshape(1, HR)
    m2[me, 10:11, :] = rpad[:, 0:128] + rpad[:, 128:256] + rpad[:, 256:384]
    w_sq = jnp.zeros((8, 128), F32)
    for j in range(NB_OUT):
        w = w_out[:, j * 128:(j + 1) * 128]
        w_sq = w_sq + jnp.sum((w * w).reshape(HR // 8, 8, 128), axis=0)
    m2[me, 13:14, :] = jnp.sum(w_sq, axis=0, keepdims=True)

    out_step(4, 0, 0)
    out_step(5, 0, 1)

    g_copy.wait()
    for b, ref in enumerate((acc, grecv)):
        s = jnp.zeros((XR, 128), F32)
        for j in range(NB_IN):
            g = ref[0:XR, j * 128:(j + 1) * 128]
            s = s + g * g
        row_sq[b * 128:(b + 1) * 128, :] = jnp.broadcast_to(jnp.sum(s, axis=1, keepdims=True), (XR, 128))

    out_step(6, 1, 0)
    out_step(7, 1, 1)

    for j in range(NB_OUT):
        g = d_out[:, j * 128:(j + 1) * 128]
        m2[me, j:j + 1, :] = jnp.sum(g * g, axis=0, keepdims=True)
    m2_out = bcast(m2, m2_send, m2_recv)
    for cp in m2_out:
        cp.start()
    for lo, n in ROWS_OUT:
        s = jnp.zeros((n, 128), F32)
        for j in range(NB_OUT):
            g = d_out[lo:lo + n, j * 128:(j + 1) * 128]
            s = s + g * g
        row_sq[256 + lo:256 + lo + n, :] = jnp.broadcast_to(jnp.sum(s, axis=1, keepdims=True), (n, 128))

    exchange_wait(m1, m1_send, m1_recv)
    exchange_wait(m2, m2_send, m2_recv)

    b2 = beta[...]
    mix = 1.0 - b2
    col = [(m1[0] + m1[2]) + (m1[4] + m1[6]), (m1[1] + m1[3]) + (m1[5] + m1[7])]
    both = ((m2[0] + m2[1]) + (m2[2] + m2[3])) + ((m2[4] + m2[5]) + (m2[6] + m2[7]))
    col.append(both[0:8, :])
    scal = jnp.sum(both[8:16, :], axis=1, keepdims=True)
    tot = [total(v) for v in col]
    norm_sq = tot[0] + tot[1] + tot[2]
    gs = jnp.minimum(1.0, cnorm[...] / jnp.sqrt(norm_sq))

    shape = [(D, FF), (D, FF), (FF, D)]
    level = [b2 * scal[k:k + 1, :] / m + mix * (gs * (gs * tot[k]) / (m * n) + EPS_ONE)
             for k, (m, n) in enumerate(shape)]

    fac = []
    for k in range(3):
        nb = NB_IN if k < 2 else NB_OUT
        old = ([ci[k:k + 1, j * 128:(j + 1) * 128] for j in range(nb)] if k < 2
               else [co[:, j * 128:(j + 1) * 128] for j in range(nb)])
        rows = []
        for j in range(nb):
            new = b2 * old[j] + mix * (gs * (gs * col[k][j:j + 1, :]) / shape[k][0] + EPS_ONE)
            if k < 2:
                cin_new[k:k + 1, j * 128:(j + 1) * 128] = new
            else:
                cout_new[:, j * 128:(j + 1) * 128] = new
            rows.append(gs * lax.rsqrt(new))
        fac.append(rows)

    def row_factor(old, sq, lvl, n):
        new = b2 * old + mix * (gs * (gs * sq) / n + EPS_ONE)
        return new, lax.rsqrt(new / lvl)

    lane = lax.broadcasted_iota(jnp.int32, (1, 128), 1)
    m3[me] = jnp.zeros((8, 128), F32)

    def pick(a, b, first):
        return jnp.where(first, a, b)

    is0 = core == 0
    for b, ref in enumerate((acc, grecv)):
        first = is0 if b == 0 else jnp.logical_not(is0)
        t = [pick(fac[0][j], fac[1][j], first) for j in range(NB_IN)]
        old = pick(ri[0:1, :], ri[1:2, :], first)
        lvl = pick(level[0], level[1], first)
        new, fr = row_factor(spread(old), row_sq[b * 128:(b + 1) * 128, :], lvl, FF)
        s = jnp.zeros((XR, 128), F32)
        for j in range(NB_IN):
            v = ref[0:XR, j * 128:(j + 1) * 128] * t[j]
            s = s + v * v
        usq = jnp.sum(s * (fr * fr), axis=0, keepdims=True)
        k = core if b == 0 else other
        m3[me, pl.ds(k, 1), :] = usq
        row_sq[b * 128:(b + 1) * 128, :] = fr
        rin_new[pl.ds(k, 1), :] = new.T[0:1, :]
    usq = jnp.zeros((1, 128), F32)
    for lo, n in ROWS_OUT:
        old = spread(rpad[:, lo:lo + 128])[0:n, :]
        new, fr = row_factor(old, row_sq[256 + lo:256 + lo + n, :], level[2], D)
        s = jnp.zeros((n, 128), F32)
        for j in range(NB_OUT):
            v = d_out[lo:lo + n, j * 128:(j + 1) * 128] * fac[2][j]
            s = s + v * v
        usq = usq + jnp.sum(s * (fr * fr), axis=0, keepdims=True)
        row_sq[256 + lo:256 + lo + n, :] = fr
        if n < 128:
            new = jnp.concatenate([new, jnp.zeros((128 - n, 128), F32)], axis=0)
        rpad[:, lo:lo + 128] = new.T[0:1, :]
    m3[me, 2:3, :] = usq
    rout_new[...] = rpad[:, 0:HR].reshape(HR)

    m3_out = bcast(m3, m3_send, m3_recv)
    for cp in m3_out:
        cp.start()

    for b, ref in enumerate((acc, grecv)):
        first = is0 if b == 0 else jnp.logical_not(is0)
        k = core if b == 0 else other
        fr = row_sq[b * 128:(b + 1) * 128, :]
        for j in range(NB_IN):
            t = pick(fac[0][j], fac[1][j], first)
            d_in[k, :, j * 128:(j + 1) * 128] = ref[0:XR, j * 128:(j + 1) * 128] * t * fr
    for lo, n in ROWS_OUT:
        fr = row_sq[256 + lo:256 + lo + n, :]
        for j in range(NB_OUT):
            c = slice(j * 128, (j + 1) * 128)
            d_out[lo:lo + n, c] = d_out[lo:lo + n, c] * fac[2][j] * fr

    exchange_wait(m3, m3_send, m3_recv)
    usum = ((m3[0] + m3[1]) + (m3[2] + m3[3])) + ((m3[4] + m3[5]) + (m3[6] + m3[7]))
    urms = jnp.sqrt(jnp.sum(usum, axis=1, keepdims=True)[0:3, :] / (D * FF))
    wrms = jnp.sqrt(scal[3:6, :] / (D * FF))
    kap = rel[...] * jnp.maximum(EPS_TWO, wrms) / jnp.maximum(1.0, urms / crms[...])
    kappa[0:3, :] = jnp.broadcast_to(kap, (3, 128))
    kappa[3:8, :] = jnp.zeros((5, 128), F32)

    for i in range(NC):
        x_send(i).wait_send()
    for cp in m1_out + m2_out + m3_out:
        cp.wait_send()


def write_kernel(d_in, d_out, w_in, w_out, rin, cin, rout, cout, kappa,
                 wi_hbm, ri_hbm, ci_hbm, wo_hbm, ro_hbm, co_hbm, st_in, st_out, sem, sem_small):
    small = [pltpu.make_async_copy(a, b, sem_small.at[n]) for n, (a, b) in enumerate(
        ((rin, ri_hbm), (cin, ci_hbm), (rout, ro_hbm), (cout, co_hbm)))]
    for cp in small:
        cp.start()
    copies = []
    for k in range(2):
        kap = kappa[k:k + 1, :]
        for h in range(2):
            r = slice(h * 64, (h + 1) * 64)
            for j in range(NB_IN):
                c = slice(j * 128, (j + 1) * 128)
                st_in[k, r, c] = w_in[k, r, c] - kap * d_in[k, r, c]
            cp = pltpu.make_async_copy(st_in.at[k, pl.ds(h * 64, 64)], wi_hbm.at[k, pl.ds(h * 64, 64)],
                                       sem.at[2 * k + h])
            cp.start()
            copies.append(cp)
    kap = kappa[2:3, :]
    for h in range(2):
        r = slice(h * 176, (h + 1) * 176)
        for j in range(NB_OUT):
            c = slice(j * 128, (j + 1) * 128)
            st_out[r, c] = w_out[r, c] - kap * d_out[r, c]
        cp = pltpu.make_async_copy(st_out.at[pl.ds(h * 176, 176)], wo_hbm.at[pl.ds(h * 176, 176)], sem.at[4 + h])
        cp.start()
        copies.append(cp)
    for cp in copies + small:
        cp.wait()


def local_step(x_norm, hid_act, dy_in, dy_out, w_in, w_out, row_in, col_in, row_out, col_out,
               beta_two, rel_step, clip_rms, clip_norm):
    hbm = pl.BlockSpec(memory_space=pltpu.HBM)
    vmem = pl.BlockSpec(memory_space=pltpu.VMEM)
    dma = pltpu.SemaphoreType.DMA
    mids = [(2, XR, FF), (HR, D), (2, XR, FF), (HR, D), (2, XR), (2, FF), (HR,), (1, D), (8, 128)]
    mid = pl.pallas_call(
        grad_kernel,
        out_shape=[pltpu.VMEM(s, F32) for s in mids],
        in_specs=[hbm] * 14,
        out_specs=[vmem] * len(mids),
        scratch_shapes=[
            pltpu.VMEM((T, XR), jnp.bfloat16), pltpu.VMEM((T, XR), jnp.bfloat16),
            pltpu.VMEM((2 * XR, KC), jnp.bfloat16), pltpu.VMEM((HR, T), jnp.bfloat16),
            pltpu.VMEM((3, KC, FF), jnp.bfloat16), pltpu.VMEM((2 * XR, FF), F32), pltpu.VMEM((XR, FF), F32),
            pltpu.VMEM((ND, 24, 128), F32), pltpu.VMEM((ND, 16, 128), F32), pltpu.VMEM((ND, 8, 128), F32),
            pltpu.VMEM((256 + 384, 128), F32), pltpu.VMEM((1, 384), F32),
            pltpu.VMEM((2, XR), F32), pltpu.VMEM((2, FF), F32), pltpu.VMEM((HR,), F32), pltpu.VMEM((1, D), F32),
            pltpu.VMEM((1, 1), F32), pltpu.VMEM((1, 1), F32), pltpu.VMEM((1, 1), F32), pltpu.VMEM((1, 1), F32),
            dma(()), dma((NC,)), dma((NC,)), dma((3,)), dma((2,)), dma((8,)), dma((NC,)), dma((NC,)), dma(()), dma(()),
            dma((ND,)), dma((ND,)), dma((ND,)), dma((ND,)), dma((ND,)), dma((ND,)),
        ],
        compiler_params=pltpu.CompilerParams(collective_id=0, has_side_effects=True, vmem_limit_bytes=46 << 20),
        name="grad_stats",
    )(x_norm, hid_act.T, dy_in, dy_out, w_in, w_out, row_in, col_in,
      row_out, col_out.reshape(1, D),
      beta_two.reshape(1, 1), rel_step.reshape(1, 1), clip_rms.reshape(1, 1), clip_norm.reshape(1, 1))
    mid = [pltpu.with_memory_space_constraint(v, pltpu.VMEM) for v in mid]
    outs = [(2, XR, FF), (2, XR), (2, FF), (HR, D), (HR,), (1, D)]
    out = pl.pallas_call(
        write_kernel,
        out_shape=[pltpu.HBM(s, F32) for s in outs],
        in_specs=[vmem] * len(mids),
        out_specs=[hbm] * len(outs),
        scratch_shapes=[pltpu.VMEM((2, XR, FF), F32), pltpu.VMEM((HR, D), F32), dma((6,)), dma((4,))],
        compiler_params=pltpu.CompilerParams(vmem_limit_bytes=12 << 20),
        name="write_weights",
    )(*mid)
    return (out[0], out[1], out[2], out[3], out[4], out[5].reshape(D))


def solution(mesh):
    in_specs = (P(None, 'tp'), P(None, 'tp'), P(), P(), P(None, 'tp', None), P('tp', None),
                P(None, 'tp'), P(), P('tp'), P(), P(), P(), P(), P())
    out_specs = (P(None, 'tp', None), P(None, 'tp'), P(), P('tp', None), P('tp'), P())
    return jax.shard_map(local_step, mesh=mesh, in_specs=in_specs, out_specs=out_specs, check_vma=False)
```

```python
import jax
import jax.numpy as jnp
from jax import lax
from jax.experimental import pallas as pl
from jax.experimental.pallas import tpu as pltpu
from jax.sharding import PartitionSpec as P

EPS_ONE = 1e-30
EPS_TWO = 1e-3
MESH = pl.DeviceIdType.MESH
F32 = jnp.float32

T = 8192
D = 1024
FF = 2816
ND = 8
XR = D // ND
HR = FF // ND
KC = 1024
NC = T // KC
L = 128
NB_IN = FF // L
NB_OUT = D // L
NP = 24
ROWS_OUT = ((0, L), (L, L), (2 * L, HR - 2 * L))
TILE = 2 * L
PIECES = ((0, 0, 0), (KC, 0, D), (2 * KC, 0, 0), (3 * KC, 0, D), (4 * KC, 1, 0), (5 * KC, 1, D), (6 * KC, 2, 0), (7 * KC, 2, D))
HEAD = 2


def total(v):
    return jnp.sum(jnp.sum(v, axis=0, keepdims=True), axis=1, keepdims=True)


def spread(row):
    return jnp.broadcast_to(row, (L, row.shape[1])).T


def grad_kernel(x_hbm, hid_hbm, dyi_hbm, dyo_hbm, wi_hbm, wo_hbm, ri_hbm, ci_hbm, ro_hbm, co_hbm,
                beta_hbm, rel_hbm, crms_hbm, cnorm_hbm,
                d_in, d_out, w_in, w_out, rin_new, cin_new, rout_new, cout_new, kappa,
                x_own, x_peer, xt0, xt1, hid, ring, acc, grecv, g2, m1, m2, m3, m4, row_sq, r_old, fac, c_old, rpad,
                ri, ci, ro, co, beta, rel, crms, cnorm,
                s_x, s_hid, s_dyo, s_dyi, s_w, s_small, xs_send, xs_recv, g_send, g_recv,
                m1_send, m1_recv, m2_send, m2_recv, m3_send, m3_recv, m4_send, m4_recv):
    me = lax.axis_index("tp")
    chip = me // 2
    core = me - 2 * chip
    other = 1 - core
    peer = 2 * chip + other
    diag = 3 - chip
    xn = chip + 1 - 2 * lax.rem(chip, 2)
    yn = lax.rem(chip + 2, 4)
    others = [2 * diag + core, 2 * diag + other, 2 * xn + core, 2 * yn + core, 2 * xn + other, 2 * yn + other, peer]

    def out_copies(p):
        k0, slot, c0 = PIECES[p]
        rows = pl.ds(k0, KC)
        return (pltpu.make_async_copy(hid_hbm.at[:, rows], hid.at[:, rows], s_hid.at[p]),
                pltpu.make_async_copy(dyo_hbm.at[rows, :], ring.at[slot, :, pl.ds(c0, D)], s_dyo.at[p]))

    def start_out(*ps):
        for p in ps:
            for cp in out_copies(p):
                cp.start()

    def dyi_copy(i):
        return pltpu.make_async_copy(dyi_hbm.at[core, pl.ds(i * KC, KC), :], ring.at[(i + 1) % 3], s_dyi.at[i])

    def x_send(i):
        c = pl.ds(i * KC, KC)
        return pltpu.make_async_remote_copy(x_own.at[c, :], x_peer.at[c, :], xs_send.at[i], xs_recv.at[i],
                                            device_id=(peer,), device_id_type=MESH)

    def bcast(buf, send, recv):
        out = [pltpu.make_async_remote_copy(buf.at[me], buf.at[me], send.at[k], recv.at[me],
                                            device_id=(dst,), device_id_type=MESH) for k, dst in enumerate(others)]
        for cp in out:
            cp.start()
        return out

    def exchange_wait(buf, send, recv):
        for k, src in reversed(list(enumerate(others))):
            pltpu.make_async_remote_copy(buf.at[src], buf.at[src], send.at[k], recv.at[src],
                                         device_id=(src,), device_id_type=MESH).wait_recv()

    start_out(0)
    x_load = pltpu.make_async_copy(x_hbm, x_own, s_x)
    x_load.start()
    start_out(1)
    dyi_copy(0).start()
    small = [pltpu.make_async_copy(a, b, s_small.at[n]) for n, (a, b) in enumerate(
        ((ri_hbm, ri), (ci_hbm, ci), (ro_hbm, ro), (co_hbm, co),
         (beta_hbm, beta), (rel_hbm, rel), (crms_hbm, crms), (cnorm_hbm, cnorm)))]
    for cp in small:
        cp.start()

    barrier = pltpu.get_barrier_semaphore()
    for dst in others:
        pl.semaphore_signal(barrier, inc=1, device_id=(dst,), device_id_type=MESH)
    rpad[...] = jnp.zeros_like(rpad)

    def wait_out(p):
        for cp in out_copies(p):
            cp.wait()

    def out_step(p, *extra):
        k0, slot, c0 = PIECES[p]
        lhs = hid[:, pl.ds(k0, KC)]
        for n in range(D // TILE):
            c = pl.ds(n * TILE, TILE)
            v = jnp.dot(lhs, ring[slot, :, pl.ds(c0 + n * TILE, TILE)], preferred_element_type=F32)
            d_out[:, c] = v if p == 0 else d_out[:, c] + v
            if n < len(extra):
                extra[n]()

    xt = (xt0, xt1)
    QT = KC // 4

    def transpose(i, n):
        rows = pl.ds(i * KC + n * QT, QT)
        cols = slice(n * QT, (n + 1) * QT)
        xt[i % 2][0:XR, cols] = x_own[rows, :].T
        xt[i % 2][XR:2 * XR, cols] = x_peer[rows, :].T

    own, both = slice(0, XR), slice(0, 2 * XR)
    blocks = [(both, n * TILE) for n in range(FF // TILE - 1)] + [(own, FF - TILE), (slice(XR, 2 * XR), FF - TILE)]

    def in_step(i):
        for n, (rows, c0) in enumerate(blocks):
            c = slice(c0, c0 + TILE)
            v = jnp.dot(xt[i % 2][rows, :], ring[(i + 1) % 3, :, c], preferred_element_type=F32)
            acc[rows, c] = v if i == 0 else acc[rows, c] + v
            if n < 4 and i + 1 < NC:
                transpose(i + 1, n)

    wait_out(0)
    out_step(0)
    dyi_copy(1).start()
    pl.semaphore_wait(barrier, ND - 1)
    x_load.wait()
    for i in range(NC):
        x_send(i).start()
    wait_out(1)
    out_step(1)
    dyi_copy(2).start()
    x_send(0).wait_recv()
    for n in range(4):
        transpose(0, n)
    for i in range(NC):
        if i + 1 < NC:
            x_send(i + 1).wait_recv()
        dyi_copy(i).wait()
        in_step(i)
        if i + 3 < NC:
            dyi_copy(i + 3).start()
        else:
            p = HEAD + 2 * (i + 3 - NC)
            start_out(p, p + 1)

    loads = [pltpu.make_async_copy(wi_hbm, w_in, s_w.at[0]), pltpu.make_async_copy(wo_hbm, w_out, s_w.at[1])]
    for cp in loads:
        cp.start()

    def stats_early():
        for j in range(NB_IN):
            g = acc[:, j * L:(j + 1) * L]
            m1[me, j:j + 1, :] = jnp.sum(g * g, axis=0, keepdims=True)
        rpad[:, 0:HR] = ro[...].reshape(1, HR)
        m1[me, NB_IN:NP, :] = jnp.zeros((NP - NB_IN, L), F32)
        m1[me, NP:26, :] = ri[...]
        m1[me, 26:27, :] = rpad[:, 0:L] + rpad[:, L:2 * L] + rpad[:, 2 * L:3 * L]
        m1[me, 27:32, :] = jnp.zeros((5, L), F32)

    for cp in small:
        cp.wait()
    wait_out(2)
    out_step(2, stats_early)
    g_copy = pltpu.make_async_remote_copy(acc.at[pl.ds(XR, XR), :], grecv, g_send, g_recv,
                                          device_id=(peer,), device_id_type=MESH)
    g_copy.start()
    m1_out = bcast(m1, m1_send, m1_recv)

    def stats_own(b, ref):
        def body():
            s = jnp.zeros((XR, L), F32)
            for j in range(NB_IN):
                c = slice(j * L, (j + 1) * L)
                g = ref[0:XR, c]
                g = g * g
                g2[b * L:(b + 1) * L, c] = g
                s = s + g
            row_sq[b * L:(b + 1) * L, :] = jnp.broadcast_to(jnp.sum(s, axis=1, keepdims=True), (XR, L))
        return body

    def old_stats():
        for k in range(2):
            r_old[k * L:(k + 1) * L, :] = spread(ri[k:k + 1, :])
            for j in range(NB_IN):
                c_old[k, j:j + 1, :] = ci[k:k + 1, j * L:(j + 1) * L]
            c_old[k, NB_IN:NP, :] = jnp.ones((NP - NB_IN, L), F32)
        for lo in (0, L, 2 * L):
            r_old[2 * L + lo:3 * L + lo, :] = spread(rpad[:, lo:lo + L])
        for j in range(NB_OUT):
            c_old[2, j:j + 1, :] = co[:, j * L:(j + 1) * L]

    wait_out(3)
    out_step(3, stats_own(0, acc))
    wait_out(4)
    out_step(4, old_stats)
    wait_out(5)
    g_copy.wait()
    out_step(5, stats_own(1, grecv))
    wait_out(6)
    out_step(6)
    wait_out(7)
    out_step(7)

    for j in range(NB_OUT):
        g = d_out[:, j * L:(j + 1) * L]
        m2[me, j:j + 1, :] = jnp.sum(g * g, axis=0, keepdims=True)
    m2_out = bcast(m2, m2_send, m2_recv)

    for lo, n in ROWS_OUT:
        s = jnp.zeros((n, L), F32)
        for j in range(NB_OUT):
            c = slice(j * L, (j + 1) * L)
            g = d_out[lo:lo + n, c]
            g = g * g
            g2[2 * L + lo:2 * L + lo + n, c] = g
            s = s + g
        row_sq[2 * L + lo:2 * L + lo + n, :] = jnp.broadcast_to(jnp.sum(s, axis=1, keepdims=True), (n, L))
    for cp in loads:
        cp.wait()
    m4[me] = jnp.zeros((8, L), F32)
    for k in range(2):
        w_sq = jnp.zeros((8, L), F32)
        for j in range(NB_IN):
            w = w_in[k, :, j * L:(j + 1) * L]
            w_sq = w_sq + jnp.sum((w * w).reshape(XR // 8, 8, L), axis=0)
        m4[me, k:k + 1, :] = jnp.sum(w_sq, axis=0, keepdims=True)
    w_sq = jnp.zeros((8, L), F32)
    for j in range(NB_OUT):
        w = w_out[:, j * L:(j + 1) * L]
        w_sq = w_sq + jnp.sum((w * w).reshape(HR // 8, 8, L), axis=0)
    m4[me, 2:3, :] = jnp.sum(w_sq, axis=0, keepdims=True)

    exchange_wait(m1, m1_send, m1_recv)
    b2 = beta[...]
    mix = 1.0 - b2
    col = [(m1[0, 0:NP] + m1[2, 0:NP]) + (m1[4, 0:NP] + m1[6, 0:NP]),
           (m1[1, 0:NP] + m1[3, 0:NP]) + (m1[5, 0:NP] + m1[7, 0:NP])]
    tail = slice(NP, 32)
    scal = ((m1[0, tail] + m1[1, tail]) + (m1[2, tail] + m1[3, tail])) + (
        (m1[4, tail] + m1[5, tail]) + (m1[6, tail] + m1[7, tail]))
    scal = jnp.sum(scal, axis=1, keepdims=True)
    tot = [total(v) for v in col]
    exchange_wait(m2, m2_send, m2_recv)
    col.append(((m2[0] + m2[1]) + (m2[2] + m2[3])) + ((m2[4] + m2[5]) + (m2[6] + m2[7])))
    tot.append(total(col[2]))
    norm_sq = tot[0] + tot[1] + tot[2]
    gs = jnp.minimum(1.0, cnorm[...] / jnp.sqrt(norm_sq))

    shape = [(D, FF), (D, FF), (FF, D)]
    level = [b2 * scal[k:k + 1, :] / m + mix * (gs * (gs * tot[k]) / (m * n) + EPS_ONE)
             for k, (m, n) in enumerate(shape)]

    for k in range(3):
        nb = NP if k < 2 else NB_OUT
        new = b2 * c_old[k, 0:nb] + mix * (gs * (gs * col[k]) / shape[k][0] + EPS_ONE)
        c_old[k, 0:nb] = new
        t = gs * lax.rsqrt(new)
        fac[k, 0:nb] = t
        fac[3 + k, 0:nb] = t * t

    def row_factor(old, rows, lvl, n):
        new = b2 * old + mix * (gs * (gs * row_sq[rows, :]) / n + EPS_ONE)
        return new, lax.rsqrt(new / lvl)

    is0 = core == 0
    ks = (core, other)
    for b in range(2):
        rows = slice(b * L, (b + 1) * L)
        lvl = jnp.where(is0 if b == 0 else jnp.logical_not(is0), level[0], level[1])
        new, fr = row_factor(r_old[pl.ds(pl.multiple_of(ks[b] * L, L), L), :], rows, lvl, FF)
        s = jnp.zeros((XR, L), F32)
        for j in range(NB_IN):
            s = s + g2[rows, j * L:(j + 1) * L] * fac[3 + ks[b], j:j + 1, :]
        m3[me, pl.ds(ks[b], 1), :] = jnp.sum(s * (fr * fr), axis=0, keepdims=True)
        row_sq[rows, :] = fr
        r_old[pl.ds(pl.multiple_of(ks[b] * L, L), L), :] = new
    usq = jnp.zeros((1, L), F32)
    for lo, n in ROWS_OUT:
        rows = slice(2 * L + lo, 2 * L + lo + n)
        new, fr = row_factor(r_old[rows, :], rows, level[2], D)
        s = jnp.zeros((n, L), F32)
        for j in range(NB_OUT):
            s = s + g2[rows, j * L:(j + 1) * L] * fac[5, j:j + 1, :]
        usq = usq + jnp.sum(s * (fr * fr), axis=0, keepdims=True)
        row_sq[rows, :] = fr
        r_old[rows, :] = new
    m3[me, 2:3, :] = usq
    m3[me, 3:4, :] = jnp.zeros((1, L), F32)
    m3_out = bcast(m3, m3_send, m3_recv)
    m4_out = bcast(m4, m4_send, m4_recv)

    for b, ref in enumerate((acc, grecv)):
        fr = row_sq[b * L:(b + 1) * L, :]
        for j in range(NB_IN):
            c = slice(j * L, (j + 1) * L)
            d_in[ks[b], :, c] = ref[0:XR, c] * fac[ks[b], j:j + 1, :] * fr
    for lo, n in ROWS_OUT:
        fr = row_sq[2 * L + lo:2 * L + lo + n, :]
        for j in range(NB_OUT):
            c = slice(j * L, (j + 1) * L)
            d_out[lo:lo + n, c] = d_out[lo:lo + n, c] * fac[2, j:j + 1, :] * fr
    for k in range(2):
        rin_new[k:k + 1, :] = r_old[k * L:(k + 1) * L, :].T[0:1, :]
        for j in range(NB_IN):
            cin_new[k:k + 1, j * L:(j + 1) * L] = c_old[k, j:j + 1, :]
    for lo in (0, L, 2 * L):
        rpad[:, lo:lo + L] = r_old[2 * L + lo:3 * L + lo, :].T[0:1, :]
    rout_new[...] = rpad[:, 0:HR].reshape(HR)
    for j in range(NB_OUT):
        cout_new[:, j * L:(j + 1) * L] = c_old[2, j:j + 1, :]

    exchange_wait(m4, m4_send, m4_recv)
    wsum = ((m4[0] + m4[1]) + (m4[2] + m4[3])) + ((m4[4] + m4[5]) + (m4[6] + m4[7]))
    wrms = jnp.sqrt(jnp.sum(wsum, axis=1, keepdims=True)[0:4, :] / (D * FF))
    step = rel[...] * jnp.maximum(EPS_TWO, wrms)
    exchange_wait(m3, m3_send, m3_recv)
    usum = ((m3[0] + m3[1]) + (m3[2] + m3[3])) + ((m3[4] + m3[5]) + (m3[6] + m3[7]))
    urms = jnp.sqrt(jnp.sum(usum, axis=1, keepdims=True) / (D * FF))
    kappa[0:4, :] = jnp.broadcast_to(step / jnp.maximum(1.0, urms / crms[...]), (4, L))
    kappa[4:8, :] = jnp.zeros((4, L), F32)

    for i in range(NC):
        x_send(i).wait_send()
    for cp in m1_out + m2_out + m3_out + m4_out:
        cp.wait_send()


def write_kernel(d_in, d_out, w_in, w_out, rin, cin, rout, cout, kappa,
                 wi_hbm, ri_hbm, ci_hbm, wo_hbm, ro_hbm, co_hbm, st_in, st_out, sem, sem_small):
    copies = []
    for k in range(2):
        kap = kappa[k:k + 1, :]
        for h in range(4):
            r = slice(h * 32, (h + 1) * 32)
            for j in range(NB_IN):
                c = slice(j * L, (j + 1) * L)
                st_in[k, r, c] = w_in[k, r, c] - kap * d_in[k, r, c]
            cp = pltpu.make_async_copy(st_in.at[k, pl.ds(h * 32, 32)], wi_hbm.at[k, pl.ds(h * 32, 32)],
                                       sem.at[4 * k + h])
            cp.start()
            copies.append(cp)
    small = [pltpu.make_async_copy(a, b, sem_small.at[n]) for n, (a, b) in enumerate(
        ((rin, ri_hbm), (cin, ci_hbm), (rout, ro_hbm), (cout, co_hbm)))]
    for cp in small:
        cp.start()
    kap = kappa[2:3, :]
    for h in range(4):
        r = slice(h * 88, (h + 1) * 88)
        for j in range(NB_OUT):
            c = slice(j * L, (j + 1) * L)
            st_out[r, c] = w_out[r, c] - kap * d_out[r, c]
        cp = pltpu.make_async_copy(st_out.at[pl.ds(h * 88, 88)], wo_hbm.at[pl.ds(h * 88, 88)], sem.at[8 + h])
        cp.start()
        copies.append(cp)
    for cp in copies + small:
        cp.wait()


def local_step(x_norm, hid_act, dy_in, dy_out, w_in, w_out, row_in, col_in, row_out, col_out,
               beta_two, rel_step, clip_rms, clip_norm):
    hbm = pl.BlockSpec(memory_space=pltpu.HBM)
    vmem = pl.BlockSpec(memory_space=pltpu.VMEM)
    dma = pltpu.SemaphoreType.DMA
    mids = [(2, XR, FF), (HR, D), (2, XR, FF), (HR, D), (2, XR), (2, FF), (HR,), (1, D), (8, L)]
    mid = pl.pallas_call(
        grad_kernel,
        out_shape=[pltpu.VMEM(s, F32) for s in mids],
        in_specs=[hbm] * 14,
        out_specs=[vmem] * len(mids),
        scratch_shapes=[
            pltpu.VMEM((T, XR), jnp.bfloat16), pltpu.VMEM((T, XR), jnp.bfloat16),
            pltpu.VMEM((2 * XR, KC), jnp.bfloat16), pltpu.VMEM((2 * XR, KC), jnp.bfloat16),
            pltpu.VMEM((HR, T), jnp.bfloat16), pltpu.VMEM((3, KC, FF), jnp.bfloat16),
            pltpu.VMEM((2 * XR, FF), F32), pltpu.VMEM((XR, FF), F32), pltpu.VMEM((2 * L + 3 * L, FF), F32),
            pltpu.VMEM((ND, 32, L), F32), pltpu.VMEM((ND, 8, L), F32), pltpu.VMEM((ND, 4, L), F32),
            pltpu.VMEM((ND, 8, L), F32), pltpu.VMEM((5 * L, L), F32), pltpu.VMEM((5 * L, L), F32),
            pltpu.VMEM((6, NP, L), F32), pltpu.VMEM((3, NP, L), F32), pltpu.VMEM((1, 3 * L), F32),
            pltpu.VMEM((2, XR), F32), pltpu.VMEM((2, FF), F32), pltpu.VMEM((HR,), F32), pltpu.VMEM((1, D), F32),
            pltpu.VMEM((1, 1), F32), pltpu.VMEM((1, 1), F32), pltpu.VMEM((1, 1), F32), pltpu.VMEM((1, 1), F32),
            dma(()), dma((len(PIECES),)), dma((len(PIECES),)), dma((NC,)), dma((2,)), dma((8,)), dma((NC,)), dma((NC,)),
            dma(()), dma(()), dma((ND,)), dma((ND,)), dma((ND,)), dma((ND,)), dma((ND,)), dma((ND,)), dma((ND,)),
            dma((ND,)),
        ],
        compiler_params=pltpu.CompilerParams(collective_id=0, has_side_effects=True, vmem_limit_bytes=50 << 20),
        name="grad_stats",
    )(x_norm, hid_act.T, dy_in, dy_out, w_in, w_out, row_in, col_in,
      row_out, col_out.reshape(1, D),
      beta_two.reshape(1, 1), rel_step.reshape(1, 1), clip_rms.reshape(1, 1), clip_norm.reshape(1, 1))
    mid = [pltpu.with_memory_space_constraint(v, pltpu.VMEM) for v in mid]
    outs = [(2, XR, FF), (2, XR), (2, FF), (HR, D), (HR,), (1, D)]
    out = pl.pallas_call(
        write_kernel,
        out_shape=[pltpu.HBM(s, F32) for s in outs],
        in_specs=[vmem] * len(mids),
        out_specs=[hbm] * len(outs),
        scratch_shapes=[pltpu.VMEM((2, XR, FF), F32), pltpu.VMEM((HR, D), F32), dma((12,)), dma((4,))],
        compiler_params=pltpu.CompilerParams(vmem_limit_bytes=12 << 20),
        name="write_weights",
    )(*mid)
    return (out[0], out[1], out[2], out[3], out[4], out[5].reshape(D))


def solution(mesh):
    in_specs = (P(None, 'tp'), P(None, 'tp'), P(), P(), P(None, 'tp', None), P('tp', None),
                P(None, 'tp'), P(), P('tp'), P(), P(), P(), P(), P())
    out_specs = (P(None, 'tp', None), P(None, 'tp'), P(), P('tp', None), P('tp'), P())
    return jax.shard_map(local_step, mesh=mesh, in_specs=in_specs, out_specs=out_specs, check_vma=False)
```

```python
import jax
import jax.numpy as jnp
from jax import lax
from jax.experimental import pallas as pl
from jax.experimental.pallas import tpu as pltpu
from jax.sharding import PartitionSpec as P

EPS_ONE = 1e-30
EPS_TWO = 1e-3
MESH = pl.DeviceIdType.MESH
F32 = jnp.float32

T = 8192
D = 1024
FF = 2816
ND = 8
XR = D // ND
HR = FF // ND
KC = 1024
NC = T // KC
L = 128
NB_IN = FF // L
NB_OUT = D // L
NP = 24
ROWS_OUT = ((0, L), (L, L), (2 * L, HR - 2 * L))
TILE = 2 * L
SLOTS = 4
PARTS_OUT = ((0, 32), (32, 64), (96, L), (224, L))
HEAD = 2
PIECES = NC - HEAD


def total(v):
    return jnp.sum(jnp.sum(v, axis=0, keepdims=True), axis=1, keepdims=True)


def spread(row):
    return jnp.broadcast_to(row, (L, row.shape[1])).T


def grad_kernel(x_hbm, hid_hbm, dyi_hbm, dyo_hbm, wi_hbm, wo_hbm, ri_hbm, ci_hbm, ro_hbm, co_hbm,
                beta_hbm, rel_hbm, crms_hbm, cnorm_hbm,
                d_in, d_out, w_in, w_out, rin_new, cin_new, rout_new, cout_new, kappa,
                x_own, x_peer, xt0, xt1, hid, ring, acc, grecv, g2, g2_out, go_send, go_recv, m1, m2, m3, m4, row_sq, r_old, fac, c_old, rpad,
                ri, ci, ro, co, beta, rel, crms, cnorm,
                s_x, s_hid, s_dyo, s_dyi, s_w, s_small, xs_send, xs_recv, hs_send, hs_recv, go_sems, g_send, g_recv,
                m1_send, m1_recv, m2_send, m2_recv, m3_send, m3_recv, m4_send, m4_recv):
    me = lax.axis_index("tp")
    chip = me // 2
    core = me - 2 * chip
    other = 1 - core
    peer = 2 * chip + other
    diag = 3 - chip
    xn = chip + 1 - 2 * lax.rem(chip, 2)
    yn = lax.rem(chip + 2, 4)
    others = [2 * diag + core, 2 * diag + other, 2 * xn + core, 2 * yn + core, 2 * xn + other, 2 * yn + other, peer]

    def token(p, who):
        return pl.multiple_of((who * HEAD + p) * KC, KC) if p < HEAD else (p + HEAD) * KC

    def kept(p):
        return p * KC if p < HEAD else (p + HEAD) * KC

    def out_copies(p):
        rows = pl.ds(token(p, core), KC)
        return (pltpu.make_async_copy(hid_hbm.at[:, rows], hid.at[:, pl.ds(kept(p), KC)], s_hid.at[p]),
                pltpu.make_async_copy(dyo_hbm.at[rows, :], ring.at[p // 2, :, pl.ds(p % 2 * D, D)], s_dyo.at[p]))

    def hid_send(p):
        return pltpu.make_async_remote_copy(hid_hbm.at[:, pl.ds(token(p, other), KC)],
                                            hid.at[:, pl.ds((HEAD + p) * KC, KC)], hs_send.at[p], hs_recv.at[p],
                                            device_id=(peer,), device_id_type=MESH)

    def start_out(*ps):
        for p in ps:
            for cp in out_copies(p):
                cp.start()

    def dyi_copy(i):
        return pltpu.make_async_copy(dyi_hbm.at[core, pl.ds(i * KC, KC), :], ring.at[(i + 1) % SLOTS], s_dyi.at[i])

    def x_send(i):
        c = pl.ds(i * KC, KC)
        return pltpu.make_async_remote_copy(x_own.at[c, :], x_peer.at[c, :], xs_send.at[i], xs_recv.at[i],
                                            device_id=(peer,), device_id_type=MESH)

    def bcast(buf, send, recv):
        out = [pltpu.make_async_remote_copy(buf.at[me], buf.at[me], send.at[k], recv.at[me],
                                            device_id=(dst,), device_id_type=MESH) for k, dst in enumerate(others)]
        for cp in out:
            cp.start()
        return out

    def exchange_wait(buf, send, recv):
        for k, src in reversed(list(enumerate(others))):
            pltpu.make_async_remote_copy(buf.at[src], buf.at[src], send.at[k], recv.at[src],
                                         device_id=(src,), device_id_type=MESH).wait_recv()

    start_out(0)
    x_load = pltpu.make_async_copy(x_hbm, x_own, s_x)
    x_load.start()
    start_out(1)
    dyi_copy(0).start()
    dyi_copy(1).start()
    small = [pltpu.make_async_copy(a, b, s_small.at[n]) for n, (a, b) in enumerate(
        ((ri_hbm, ri), (ci_hbm, ci), (ro_hbm, ro), (co_hbm, co),
         (beta_hbm, beta), (rel_hbm, rel), (crms_hbm, crms), (cnorm_hbm, cnorm)))]
    for cp in small:
        cp.start()

    barrier = pltpu.get_barrier_semaphore()
    for dst in others:
        pl.semaphore_signal(barrier, inc=1, device_id=(dst,), device_id_type=MESH)
    rpad[...] = jnp.zeros_like(rpad)

    def wait_out(p):
        for cp in out_copies(p):
            cp.wait()

    def out_step(p, *extra):
        for n in range(D // TILE):
            c = pl.ds(n * TILE, TILE)
            v = jnp.dot(hid[:, pl.ds(kept(p), KC)], ring[p // 2, :, pl.ds(p % 2 * D + n * TILE, TILE)],
                        preferred_element_type=F32)
            if p == HEAD:
                v = v + go_recv[:, c]
            d_out[:, c] = v if p == 0 else d_out[:, c] + v
            if n < len(extra):
                extra[n]()

    def partner_step(p):
        for n in range(D // TILE):
            c = pl.ds(n * TILE, TILE)
            v = jnp.dot(hid[:, pl.ds((HEAD + p) * KC, KC)], ring[0, :, pl.ds(p * D + n * TILE, TILE)],
                        preferred_element_type=F32)
            go_send[:, c] = v if p == 0 else go_send[:, c] + v

    xt = (xt0, xt1)
    QT = KC // 4

    def transpose(i, n):
        rows = pl.ds(i * KC + n * QT, QT)
        cols = slice(n * QT, (n + 1) * QT)
        xt[i % 2][0:XR, cols] = x_own[rows, :].T
        xt[i % 2][XR:2 * XR, cols] = x_peer[rows, :].T

    own, both = slice(0, XR), slice(0, 2 * XR)
    blocks = [(both, n * TILE) for n in range(FF // TILE - 1)] + [(own, FF - TILE), (slice(XR, 2 * XR), FF - TILE)]

    def in_step(i):
        for n, (rows, c0) in enumerate(blocks):
            c = slice(c0, c0 + TILE)
            v = jnp.dot(xt[i % 2][rows, :], ring[(i + 1) % SLOTS, :, c], preferred_element_type=F32)
            acc[rows, c] = v if i == 0 else acc[rows, c] + v
            if n < 4 and i + 1 < NC:
                transpose(i + 1, n)

    go_copy = pltpu.make_async_remote_copy(go_send, go_recv, go_sems.at[0], go_sems.at[1],
                                           device_id=(peer,), device_id_type=MESH)
    pl.semaphore_wait(barrier, ND - 1)
    for p in range(HEAD):
        hid_send(p).start()
    wait_out(0)
    out_step(0)
    x_load.wait()
    for i in range(NC):
        x_send(i).start()
    dyi_copy(2).start()
    wait_out(1)
    out_step(1)
    for p in range(HEAD):
        hid_send(p).wait_recv()
        partner_step(p)
    dyi_copy(3).start()
    x_send(0).wait_recv()
    for n in range(4):
        transpose(0, n)
    for i in range(NC):
        if i + 1 < NC:
            x_send(i + 1).wait_recv()
        dyi_copy(i).wait()
        in_step(i)
        if i == 0:
            go_copy.start()
        if i in (1, 3):
            dyi_copy(i + 3).start()
            dyi_copy(i + 4).start()
        if i == NC - 3:
            start_out(2, 3, 4, 5)

    loads = [pltpu.make_async_copy(wi_hbm, w_in, s_w.at[0]), pltpu.make_async_copy(wo_hbm, w_out, s_w.at[1])]
    for cp in loads:
        cp.start()

    def stats_early():
        for j in range(NB_IN):
            g = acc[:, j * L:(j + 1) * L]
            m1[me, j:j + 1, :] = jnp.sum(g * g, axis=0, keepdims=True)
        rpad[:, 0:HR] = ro[...].reshape(1, HR)
        m1[me, NB_IN:NP, :] = jnp.zeros((NP - NB_IN, L), F32)
        m1[me, NP:26, :] = ri[...]
        m1[me, 26:27, :] = rpad[:, 0:L] + rpad[:, L:2 * L] + rpad[:, 2 * L:3 * L]
        m1[me, 27:32, :] = jnp.zeros((5, L), F32)

    for cp in small:
        cp.wait()
    wait_out(2)
    go_copy.wait()
    g_copy = pltpu.make_async_remote_copy(acc.at[pl.ds(XR, XR), :], grecv, g_send, g_recv,
                                          device_id=(peer,), device_id_type=MESH)
    g_copy.start()
    out_step(2, stats_early)
    m1_out = bcast(m1, m1_send, m1_recv)

    def stats_own(b, ref):
        def body():
            s = jnp.zeros((XR, L), F32)
            for j in range(NB_IN):
                c = slice(j * L, (j + 1) * L)
                g = ref[0:XR, c]
                g = g * g
                g2[b * L:(b + 1) * L, c] = g
                s = s + g
            row_sq[b * L:(b + 1) * L, :] = jnp.broadcast_to(jnp.sum(s, axis=1, keepdims=True), (XR, L))
        return body

    def old_stats():
        for k in range(2):
            r_old[k * L:(k + 1) * L, :] = spread(ri[k:k + 1, :])
            for j in range(NB_IN):
                c_old[k, j:j + 1, :] = ci[k:k + 1, j * L:(j + 1) * L]
            c_old[k, NB_IN:NP, :] = jnp.ones((NP - NB_IN, L), F32)
        for lo in (0, L, 2 * L):
            r_old[2 * L + lo:3 * L + lo, :] = spread(rpad[:, lo:lo + L])
        for j in range(NB_OUT):
            c_old[2, j:j + 1, :] = co[:, j * L:(j + 1) * L]

    wait_out(3)
    out_step(3, stats_own(0, acc))
    wait_out(4)
    out_step(4, old_stats)
    wait_out(5)
    out_step(5)

    for j in range(NB_OUT):
        g = d_out[:, j * L:(j + 1) * L]
        m2[me, j:j + 1, :] = jnp.sum(g * g, axis=0, keepdims=True)
    m2_out = bcast(m2, m2_send, m2_recv)

    for lo, n in ROWS_OUT:
        s = jnp.zeros((n, L), F32)
        for j in range(NB_OUT):
            c = slice(j * L, (j + 1) * L)
            g = d_out[lo:lo + n, c]
            g = g * g
            g2_out[lo:lo + n, c] = g
            s = s + g
        row_sq[2 * L + lo:2 * L + lo + n, :] = jnp.broadcast_to(jnp.sum(s, axis=1, keepdims=True), (n, L))
    g_copy.wait()
    stats_own(1, grecv)()
    for cp in loads:
        cp.wait()
    m4[me] = jnp.zeros((8, L), F32)
    for k in range(2):
        w_sq = jnp.zeros((8, L), F32)
        for j in range(NB_IN):
            w = w_in[k, :, j * L:(j + 1) * L]
            w_sq = w_sq + jnp.sum((w * w).reshape(XR // 8, 8, L), axis=0)
        m4[me, k:k + 1, :] = jnp.sum(w_sq, axis=0, keepdims=True)
    w_sq = jnp.zeros((8, L), F32)
    for j in range(NB_OUT):
        w = w_out[:, j * L:(j + 1) * L]
        w_sq = w_sq + jnp.sum((w * w).reshape(HR // 8, 8, L), axis=0)
    m4[me, 2:3, :] = jnp.sum(w_sq, axis=0, keepdims=True)
    m4_out = bcast(m4, m4_send, m4_recv)

    exchange_wait(m1, m1_send, m1_recv)
    b2 = beta[...]
    mix = 1.0 - b2
    col = [(m1[0, 0:NP] + m1[2, 0:NP]) + (m1[4, 0:NP] + m1[6, 0:NP]),
           (m1[1, 0:NP] + m1[3, 0:NP]) + (m1[5, 0:NP] + m1[7, 0:NP])]
    tail = slice(NP, 32)
    scal = ((m1[0, tail] + m1[1, tail]) + (m1[2, tail] + m1[3, tail])) + (
        (m1[4, tail] + m1[5, tail]) + (m1[6, tail] + m1[7, tail]))
    scal = jnp.sum(scal, axis=1, keepdims=True)
    tot = [total(v) for v in col]
    exchange_wait(m2, m2_send, m2_recv)
    col.append(((m2[0] + m2[1]) + (m2[2] + m2[3])) + ((m2[4] + m2[5]) + (m2[6] + m2[7])))
    tot.append(total(col[2]))
    norm_sq = tot[0] + tot[1] + tot[2]
    gs = jnp.minimum(1.0, cnorm[...] / jnp.sqrt(norm_sq))

    shape = [(D, FF), (D, FF), (FF, D)]
    level = [b2 * scal[k:k + 1, :] / m + mix * (gs * (gs * tot[k]) / (m * n) + EPS_ONE)
             for k, (m, n) in enumerate(shape)]

    for k in range(3):
        nb = NP if k < 2 else NB_OUT
        new = b2 * c_old[k, 0:nb] + mix * (gs * (gs * col[k]) / shape[k][0] + EPS_ONE)
        c_old[k, 0:nb] = new
        t = gs * lax.rsqrt(new)
        fac[k, 0:nb] = t
        fac[3 + k, 0:nb] = t * t

    def row_factor(old, rows, lvl, n):
        new = b2 * old + mix * (gs * (gs * row_sq[rows, :]) / n + EPS_ONE)
        return new, lax.rsqrt(new / lvl)

    is0 = core == 0
    ks = (core, other)
    for b in range(2):
        rows = slice(b * L, (b + 1) * L)
        lvl = jnp.where(is0 if b == 0 else jnp.logical_not(is0), level[0], level[1])
        new, fr = row_factor(r_old[pl.ds(pl.multiple_of(ks[b] * L, L), L), :], rows, lvl, FF)
        s = jnp.zeros((XR, L), F32)
        for j in range(NB_IN):
            s = s + g2[rows, j * L:(j + 1) * L] * fac[3 + ks[b], j:j + 1, :]
        m3[me, pl.ds(ks[b], 1), :] = jnp.sum(s * (fr * fr), axis=0, keepdims=True)
        row_sq[rows, :] = fr
        r_old[pl.ds(pl.multiple_of(ks[b] * L, L), L), :] = new
    usq = jnp.zeros((1, L), F32)
    for lo, n in ROWS_OUT:
        rows = slice(2 * L + lo, 2 * L + lo + n)
        new, fr = row_factor(r_old[rows, :], rows, level[2], D)
        s = jnp.zeros((n, L), F32)
        for j in range(NB_OUT):
            s = s + g2_out[lo:lo + n, j * L:(j + 1) * L] * fac[5, j:j + 1, :]
        usq = usq + jnp.sum(s * (fr * fr), axis=0, keepdims=True)
        row_sq[rows, :] = fr
        r_old[rows, :] = new
    m3[me, 2:3, :] = usq
    m3[me, 3:4, :] = jnp.zeros((1, L), F32)
    m3_out = bcast(m3, m3_send, m3_recv)

    for b, ref in enumerate((acc, grecv)):
        fr = row_sq[b * L:(b + 1) * L, :]
        for j in range(NB_IN):
            c = slice(j * L, (j + 1) * L)
            d_in[ks[b], :, c] = ref[0:XR, c] * fac[ks[b], j:j + 1, :] * fr
    for lo, n in ROWS_OUT:
        fr = row_sq[2 * L + lo:2 * L + lo + n, :]
        for j in range(NB_OUT):
            c = slice(j * L, (j + 1) * L)
            d_out[lo:lo + n, c] = d_out[lo:lo + n, c] * fac[2, j:j + 1, :] * fr
    for k in range(2):
        rin_new[k:k + 1, :] = r_old[k * L:(k + 1) * L, :].T[0:1, :]
        for j in range(NB_IN):
            cin_new[k:k + 1, j * L:(j + 1) * L] = c_old[k, j:j + 1, :]
    for lo in (0, L, 2 * L):
        rpad[:, lo:lo + L] = r_old[2 * L + lo:3 * L + lo, :].T[0:1, :]
    rout_new[...] = rpad[:, 0:HR].reshape(HR)
    for j in range(NB_OUT):
        cout_new[:, j * L:(j + 1) * L] = c_old[2, j:j + 1, :]

    exchange_wait(m4, m4_send, m4_recv)
    wsum = ((m4[0] + m4[1]) + (m4[2] + m4[3])) + ((m4[4] + m4[5]) + (m4[6] + m4[7]))
    wrms = jnp.sqrt(jnp.sum(wsum, axis=1, keepdims=True)[0:4, :] / (D * FF))
    step = rel[...] * jnp.maximum(EPS_TWO, wrms)
    exchange_wait(m3, m3_send, m3_recv)
    usum = ((m3[0] + m3[1]) + (m3[2] + m3[3])) + ((m3[4] + m3[5]) + (m3[6] + m3[7]))
    urms = jnp.sqrt(jnp.sum(usum, axis=1, keepdims=True) / (D * FF))
    kappa[0:4, :] = jnp.broadcast_to(step / jnp.maximum(1.0, urms / crms[...]), (4, L))
    kappa[4:8, :] = jnp.zeros((4, L), F32)

    for i in range(NC):
        x_send(i).wait_send()
    for p in range(HEAD):
        hid_send(p).wait_send()
    for cp in m1_out + m2_out + m3_out + m4_out:
        cp.wait_send()


def write_kernel(d_in, d_out, w_in, w_out, rin, cin, rout, cout, kappa,
                 wi_hbm, ri_hbm, ci_hbm, wo_hbm, ro_hbm, co_hbm, st_in, st_out, sem, sem_small):
    copies = []

    def put(src, dst, s):
        cp = pltpu.make_async_copy(src, dst, s)
        cp.start()
        copies.append(cp)

    n = len(copies)
    for lo, h in PARTS_OUT:
        r = slice(lo, lo + h)
        for j in range(NB_OUT):
            c = slice(j * L, (j + 1) * L)
            st_out[r, c] = w_out[r, c] - kappa[2:3, :] * d_out[r, c]
        put(st_out.at[pl.ds(lo, h)], wo_hbm.at[pl.ds(lo, h)], sem.at[n])
        n += 1
    for k in range(2):
        for lo in range(0, XR, XR // 4):
            h = XR // 4
            r = slice(lo, lo + h)
            for j in range(NB_IN):
                c = slice(j * L, (j + 1) * L)
                st_in[k, r, c] = w_in[k, r, c] - kappa[k:k + 1, :] * d_in[k, r, c]
            put(st_in.at[k, pl.ds(lo, h)], wi_hbm.at[k, pl.ds(lo, h)], sem.at[n])
            n += 1
        if k == 0:
            for m, (a, b) in enumerate(((rin, ri_hbm), (cin, ci_hbm), (rout, ro_hbm), (cout, co_hbm))):
                put(a, b, sem_small.at[m])
    for cp in copies:
        cp.wait()


def local_step(x_norm, hid_act, dy_in, dy_out, w_in, w_out, row_in, col_in, row_out, col_out,
               beta_two, rel_step, clip_rms, clip_norm):
    hbm = pl.BlockSpec(memory_space=pltpu.HBM)
    vmem = pl.BlockSpec(memory_space=pltpu.VMEM)
    dma = pltpu.SemaphoreType.DMA
    mids = [(2, XR, FF), (HR, D), (2, XR, FF), (HR, D), (2, XR), (2, FF), (HR,), (1, D), (8, L)]
    mid = pl.pallas_call(
        grad_kernel,
        out_shape=[pltpu.VMEM(s, F32) for s in mids],
        in_specs=[hbm] * 14,
        out_specs=[vmem] * len(mids),
        scratch_shapes=[
            pltpu.VMEM((T, XR), jnp.bfloat16), pltpu.VMEM((T, XR), jnp.bfloat16),
            pltpu.VMEM((2 * XR, KC), jnp.bfloat16), pltpu.VMEM((2 * XR, KC), jnp.bfloat16),
            pltpu.VMEM((HR, T), jnp.bfloat16), pltpu.VMEM((SLOTS, KC, FF), jnp.bfloat16),
            pltpu.VMEM((2 * XR, FF), F32), pltpu.VMEM((XR, FF), F32), pltpu.VMEM((2 * L, FF), F32), pltpu.VMEM((HR, D), F32),
            pltpu.VMEM((HR, D), F32), pltpu.VMEM((HR, D), F32),
            pltpu.VMEM((ND, 32, L), F32), pltpu.VMEM((ND, 8, L), F32), pltpu.VMEM((ND, 4, L), F32),
            pltpu.VMEM((ND, 8, L), F32), pltpu.VMEM((5 * L, L), F32), pltpu.VMEM((5 * L, L), F32),
            pltpu.VMEM((6, NP, L), F32), pltpu.VMEM((3, NP, L), F32), pltpu.VMEM((1, 3 * L), F32),
            pltpu.VMEM((2, XR), F32), pltpu.VMEM((2, FF), F32), pltpu.VMEM((HR,), F32), pltpu.VMEM((1, D), F32),
            pltpu.VMEM((1, 1), F32), pltpu.VMEM((1, 1), F32), pltpu.VMEM((1, 1), F32), pltpu.VMEM((1, 1), F32),
            dma(()), dma((PIECES,)), dma((PIECES,)), dma((NC,)), dma((2,)), dma((8,)), dma((NC,)), dma((NC,)),
            dma((HEAD,)), dma((HEAD,)), dma((2,)),
            dma(()), dma(()), dma((ND,)), dma((ND,)), dma((ND,)), dma((ND,)), dma((ND,)), dma((ND,)), dma((ND,)),
            dma((ND,)),
        ],
        compiler_params=pltpu.CompilerParams(collective_id=0, has_side_effects=True, vmem_limit_bytes=52 << 20),
        name="grad_stats",
    )(x_norm, hid_act.T, dy_in, dy_out, w_in, w_out, row_in, col_in,
      row_out, col_out.reshape(1, D),
      beta_two.reshape(1, 1), rel_step.reshape(1, 1), clip_rms.reshape(1, 1), clip_norm.reshape(1, 1))
    mid = [pltpu.with_memory_space_constraint(v, pltpu.VMEM) for v in mid]
    outs = [(2, XR, FF), (2, XR), (2, FF), (HR, D), (HR,), (1, D)]
    out = pl.pallas_call(
        write_kernel,
        out_shape=[pltpu.HBM(s, F32) for s in outs],
        in_specs=[vmem] * len(mids),
        out_specs=[hbm] * len(outs),
        scratch_shapes=[pltpu.VMEM((2, XR, FF), F32), pltpu.VMEM((HR, D), F32), dma((12,)), dma((4,))],
        compiler_params=pltpu.CompilerParams(vmem_limit_bytes=12 << 20),
        name="write_weights",
    )(*mid)
    return (out[0], out[1], out[2], out[3], out[4], out[5].reshape(D))


def solution(mesh):
    in_specs = (P(None, 'tp'), P(None, 'tp'), P(), P(), P(None, 'tp', None), P('tp', None),
                P(None, 'tp'), P(), P('tp'), P(), P(), P(), P(), P())
    out_specs = (P(None, 'tp', None), P(None, 'tp'), P(), P('tp', None), P('tp'), P())
    return jax.shard_map(local_step, mesh=mesh, in_specs=in_specs, out_specs=out_specs, check_vma=False)
```

```python
import jax
import jax.numpy as jnp
from jax import lax
from jax.experimental import pallas as pl
from jax.experimental.pallas import tpu as pltpu
from jax.sharding import PartitionSpec as P

EPS_ONE = 1e-30
EPS_TWO = 1e-3
MESH = pl.DeviceIdType.MESH
F32 = jnp.float32

T = 8192
D = 1024
FF = 2816
ND = 8
XR = D // ND
HR = FF // ND
KC = 1024
NC = T // KC
L = 128
NB_IN = FF // L
NB_OUT = D // L
NP = 24
ROWS_OUT = ((0, L), (L, L), (2 * L, HR - 2 * L))
TILE = 2 * L
SLOTS = 4
PARTS_OUT = ((0, 32), (32, 64), (96, L), (224, L))
HEAD = 2
PIECES = NC - HEAD


def total(v):
    return jnp.sum(jnp.sum(v, axis=0, keepdims=True), axis=1, keepdims=True)


def spread(row):
    return jnp.broadcast_to(row, (L, row.shape[1])).T


def grad_kernel(x_hbm, hid_hbm, dyi_hbm, dyo_hbm, wi_hbm, wo_hbm, ri_hbm, ci_hbm, ro_hbm, co_hbm,
                beta_hbm, rel_hbm, crms_hbm, cnorm_hbm,
                d_in, d_out, w_in, w_out, rin_new, cin_new, rout_new, cout_new, kappa,
                x_own, x_peer, xt0, xt1, hid, ring, acc, grecv, g2, g2_out, go_send, go_recv, m1, m2, m3, m4, row_sq, r_old, fac, c_old, rpad,
                ri, ci, ro, co, beta, rel, crms, cnorm,
                s_x, s_hid, s_dyo, s_dyi, s_w, s_small, xs_send, xs_recv, hs_send, hs_recv, go_sems, g_send, g_recv,
                m1_send, m1_recv, m2_send, m2_recv, m3_send, m3_recv, m4_send, m4_recv):
    me = lax.axis_index("tp")
    chip = me // 2
    core = me - 2 * chip
    other = 1 - core
    peer = 2 * chip + other
    diag = 3 - chip
    xn = chip + 1 - 2 * lax.rem(chip, 2)
    yn = lax.rem(chip + 2, 4)
    others = [2 * diag + core, 2 * diag + other, 2 * xn + core, 2 * yn + core, 2 * xn + other, 2 * yn + other, peer]

    def token(p, who):
        return pl.multiple_of((who * HEAD + p) * KC, KC) if p < HEAD else (p + HEAD) * KC

    def kept(p):
        return p * KC if p < HEAD else (p + HEAD) * KC

    def out_copies(p):
        rows = pl.ds(token(p, core), KC)
        return (pltpu.make_async_copy(hid_hbm.at[:, rows], hid.at[:, pl.ds(kept(p), KC)], s_hid.at[p]),
                pltpu.make_async_copy(dyo_hbm.at[rows, :], ring.at[p // 2, :, pl.ds(p % 2 * D, D)], s_dyo.at[p]))

    def hid_send(p):
        return pltpu.make_async_remote_copy(hid_hbm.at[:, pl.ds(token(p, other), KC)],
                                            hid.at[:, pl.ds((HEAD + p) * KC, KC)], hs_send.at[p], hs_recv.at[p],
                                            device_id=(peer,), device_id_type=MESH)

    def start_out(*ps):
        for p in ps:
            for cp in out_copies(p):
                cp.start()

    def dyi_copy(i):
        return pltpu.make_async_copy(dyi_hbm.at[core, pl.ds(i * KC, KC), :], ring.at[(i + 1) % SLOTS], s_dyi.at[i])

    def x_send(i):
        c = pl.ds(i * KC, KC)
        return pltpu.make_async_remote_copy(x_own.at[c, :], x_peer.at[c, :], xs_send.at[i], xs_recv.at[i],
                                            device_id=(peer,), device_id_type=MESH)

    def bcast(buf, send, recv):
        out = [pltpu.make_async_remote_copy(buf.at[me], buf.at[me], send.at[k], recv.at[me],
                                            device_id=(dst,), device_id_type=MESH) for k, dst in enumerate(others)]
        for cp in out:
            cp.start()
        return out

    def exchange_wait(buf, send, recv):
        for k, src in reversed(list(enumerate(others))):
            pltpu.make_async_remote_copy(buf.at[src], buf.at[src], send.at[k], recv.at[src],
                                         device_id=(src,), device_id_type=MESH).wait_recv()

    x_loads = [pltpu.make_async_copy(x_hbm.at[r, :], x_own.at[r, :], s_x.at[n])
               for n, r in enumerate((pl.ds(0, KC), pl.ds(KC, T - KC)))]
    start_out(0)
    x_loads[0].start()
    start_out(1)
    dyi_copy(0).start()
    x_loads[1].start()
    dyi_copy(1).start()
    small = [pltpu.make_async_copy(a, b, s_small.at[n]) for n, (a, b) in enumerate(
        ((ri_hbm, ri), (ci_hbm, ci), (ro_hbm, ro), (co_hbm, co),
         (beta_hbm, beta), (rel_hbm, rel), (crms_hbm, crms), (cnorm_hbm, cnorm)))]
    for cp in small:
        cp.start()

    barrier = pltpu.get_barrier_semaphore()
    for dst in others:
        pl.semaphore_signal(barrier, inc=1, device_id=(dst,), device_id_type=MESH)
    rpad[...] = jnp.zeros_like(rpad)

    def wait_out(p):
        for cp in out_copies(p):
            cp.wait()

    def out_step(p, *extra):
        for n in range(D // TILE):
            c = pl.ds(n * TILE, TILE)
            v = jnp.dot(hid[:, pl.ds(kept(p), KC)], ring[p // 2, :, pl.ds(p % 2 * D + n * TILE, TILE)],
                        preferred_element_type=F32)
            if p == HEAD:
                v = v + go_recv[:, c]
            d_out[:, c] = v if p == 0 else d_out[:, c] + v
            if n < len(extra):
                extra[n]()

    def partner_step(p, turn=False):
        for n in range(D // TILE):
            c = pl.ds(n * TILE, TILE)
            v = jnp.dot(hid[:, pl.ds((HEAD + p) * KC, KC)], ring[0, :, pl.ds(p * D + n * TILE, TILE)],
                        preferred_element_type=F32)
            go_send[:, c] = v if p == 0 else go_send[:, c] + v
            if turn:
                transpose(1, n)

    xt = (xt0, xt1)
    QT = KC // 4

    def transpose(i, n):
        rows = pl.ds(i * KC + n * QT, QT)
        cols = slice(n * QT, (n + 1) * QT)
        xt[i % 2][0:XR, cols] = x_own[rows, :].T
        xt[i % 2][XR:2 * XR, cols] = x_peer[rows, :].T

    own, both = slice(0, XR), slice(0, 2 * XR)
    blocks = [(both, n * TILE) for n in range(FF // TILE - 1)] + [(own, FF - TILE), (slice(XR, 2 * XR), FF - TILE)]

    def in_step(i):
        for n, (rows, c0) in enumerate(blocks):
            c = slice(c0, c0 + TILE)
            v = jnp.dot(xt[i % 2][rows, :], ring[(i + 1) % SLOTS, :, c], preferred_element_type=F32)
            acc[rows, c] = v if i == 0 else acc[rows, c] + v
            if n < 4 and 0 < i < NC - 1:
                transpose(i + 1, n)

    go_copy = pltpu.make_async_remote_copy(go_send, go_recv, go_sems.at[0], go_sems.at[1],
                                           device_id=(peer,), device_id_type=MESH)
    pl.semaphore_wait(barrier, ND - 1)
    x_loads[0].wait()
    x_send(0).start()
    wait_out(0)
    out_step(0)
    dyi_copy(2).start()
    for p in range(HEAD):
        hid_send(p).start()
    wait_out(1)
    out_step(1)
    x_send(0).wait_recv()
    for n in range(4):
        transpose(0, n)
    for i in range(NC):
        if 0 < i < NC - 1:
            x_send(i + 1).wait_recv()
        dyi_copy(i).wait()
        in_step(i)
        if i == 0:
            x_loads[1].wait()
            for k in range(1, NC):
                x_send(k).start()
            hid_send(0).wait_recv()
            partner_step(0)
            hid_send(1).wait_recv()
            x_send(1).wait_recv()
            partner_step(1, True)
            dyi_copy(3).start()
        if i == 1:
            go_copy.start()
        if i in (1, 3):
            dyi_copy(i + 3).start()
            dyi_copy(i + 4).start()
        if i == NC - 3:
            start_out(2, 3, 4, 5)

    loads = [pltpu.make_async_copy(wi_hbm, w_in, s_w.at[0]), pltpu.make_async_copy(wo_hbm, w_out, s_w.at[1])]
    for cp in loads:
        cp.start()

    def stats_early():
        for j in range(NB_IN):
            g = acc[:, j * L:(j + 1) * L]
            m1[me, j:j + 1, :] = jnp.sum(g * g, axis=0, keepdims=True)
        rpad[:, 0:HR] = ro[...].reshape(1, HR)
        m1[me, NB_IN:NP, :] = jnp.zeros((NP - NB_IN, L), F32)
        m1[me, NP:26, :] = ri[...]
        m1[me, 26:27, :] = rpad[:, 0:L] + rpad[:, L:2 * L] + rpad[:, 2 * L:3 * L]
        m1[me, 27:32, :] = jnp.zeros((5, L), F32)

    for cp in small:
        cp.wait()
    wait_out(2)
    go_copy.wait()
    g_copy = pltpu.make_async_remote_copy(acc.at[pl.ds(XR, XR), :], grecv, g_send, g_recv,
                                          device_id=(peer,), device_id_type=MESH)
    g_copy.start()
    out_step(2, stats_early)
    m1_out = bcast(m1, m1_send, m1_recv)

    def stats_own(b, ref):
        def body():
            s = jnp.zeros((XR, L), F32)
            for j in range(NB_IN):
                c = slice(j * L, (j + 1) * L)
                g = ref[0:XR, c]
                g = g * g
                g2[b * L:(b + 1) * L, c] = g
                s = s + g
            row_sq[b * L:(b + 1) * L, :] = jnp.broadcast_to(jnp.sum(s, axis=1, keepdims=True), (XR, L))
        return body

    def old_stats():
        for k in range(2):
            r_old[k * L:(k + 1) * L, :] = spread(ri[k:k + 1, :])
            for j in range(NB_IN):
                c_old[k, j:j + 1, :] = ci[k:k + 1, j * L:(j + 1) * L]
            c_old[k, NB_IN:NP, :] = jnp.ones((NP - NB_IN, L), F32)
        for lo in (0, L, 2 * L):
            r_old[2 * L + lo:3 * L + lo, :] = spread(rpad[:, lo:lo + L])
        for j in range(NB_OUT):
            c_old[2, j:j + 1, :] = co[:, j * L:(j + 1) * L]

    wait_out(3)
    out_step(3, stats_own(0, acc))
    wait_out(4)
    out_step(4, old_stats)
    wait_out(5)
    out_step(5)

    for j in range(NB_OUT):
        g = d_out[:, j * L:(j + 1) * L]
        m2[me, j:j + 1, :] = jnp.sum(g * g, axis=0, keepdims=True)
    m2_out = bcast(m2, m2_send, m2_recv)

    for lo, n in ROWS_OUT:
        s = jnp.zeros((n, L), F32)
        for j in range(NB_OUT):
            c = slice(j * L, (j + 1) * L)
            g = d_out[lo:lo + n, c]
            g = g * g
            g2_out[lo:lo + n, c] = g
            s = s + g
        row_sq[2 * L + lo:2 * L + lo + n, :] = jnp.broadcast_to(jnp.sum(s, axis=1, keepdims=True), (n, L))
    g_copy.wait()
    stats_own(1, grecv)()
    for cp in loads:
        cp.wait()
    m4[me] = jnp.zeros((8, L), F32)
    for k in range(2):
        w_sq = jnp.zeros((8, L), F32)
        for j in range(NB_IN):
            w = w_in[k, :, j * L:(j + 1) * L]
            w_sq = w_sq + jnp.sum((w * w).reshape(XR // 8, 8, L), axis=0)
        m4[me, k:k + 1, :] = jnp.sum(w_sq, axis=0, keepdims=True)
    w_sq = jnp.zeros((8, L), F32)
    for j in range(NB_OUT):
        w = w_out[:, j * L:(j + 1) * L]
        w_sq = w_sq + jnp.sum((w * w).reshape(HR // 8, 8, L), axis=0)
    m4[me, 2:3, :] = jnp.sum(w_sq, axis=0, keepdims=True)
    m4_out = bcast(m4, m4_send, m4_recv)

    exchange_wait(m1, m1_send, m1_recv)
    b2 = beta[...]
    mix = 1.0 - b2
    col = [(m1[0, 0:NP] + m1[2, 0:NP]) + (m1[4, 0:NP] + m1[6, 0:NP]),
           (m1[1, 0:NP] + m1[3, 0:NP]) + (m1[5, 0:NP] + m1[7, 0:NP])]
    tail = slice(NP, 32)
    scal = ((m1[0, tail] + m1[1, tail]) + (m1[2, tail] + m1[3, tail])) + (
        (m1[4, tail] + m1[5, tail]) + (m1[6, tail] + m1[7, tail]))
    scal = jnp.sum(scal, axis=1, keepdims=True)
    tot = [total(v) for v in col]
    exchange_wait(m2, m2_send, m2_recv)
    col.append(((m2[0] + m2[1]) + (m2[2] + m2[3])) + ((m2[4] + m2[5]) + (m2[6] + m2[7])))
    tot.append(total(col[2]))
    norm_sq = tot[0] + tot[1] + tot[2]
    gs = jnp.minimum(1.0, cnorm[...] / jnp.sqrt(norm_sq))

    shape = [(D, FF), (D, FF), (FF, D)]
    level = [b2 * scal[k:k + 1, :] / m + mix * (gs * (gs * tot[k]) / (m * n) + EPS_ONE)
             for k, (m, n) in enumerate(shape)]

    for k in range(3):
        nb = NP if k < 2 else NB_OUT
        new = b2 * c_old[k, 0:nb] + mix * (gs * (gs * col[k]) / shape[k][0] + EPS_ONE)
        c_old[k, 0:nb] = new
        t = gs * lax.rsqrt(new)
        fac[k, 0:nb] = t
        fac[3 + k, 0:nb] = t * t

    def row_factor(old, rows, lvl, n):
        new = b2 * old + mix * (gs * (gs * row_sq[rows, :]) / n + EPS_ONE)
        return new, lax.rsqrt(new / lvl)

    is0 = core == 0
    ks = (core, other)
    for b in range(2):
        rows = slice(b * L, (b + 1) * L)
        lvl = jnp.where(is0 if b == 0 else jnp.logical_not(is0), level[0], level[1])
        new, fr = row_factor(r_old[pl.ds(pl.multiple_of(ks[b] * L, L), L), :], rows, lvl, FF)
        s = jnp.zeros((XR, L), F32)
        for j in range(NB_IN):
            s = s + g2[rows, j * L:(j + 1) * L] * fac[3 + ks[b], j:j + 1, :]
        m3[me, pl.ds(ks[b], 1), :] = jnp.sum(s * (fr * fr), axis=0, keepdims=True)
        row_sq[rows, :] = fr
        r_old[pl.ds(pl.multiple_of(ks[b] * L, L), L), :] = new
    usq = jnp.zeros((1, L), F32)
    for lo, n in ROWS_OUT:
        rows = slice(2 * L + lo, 2 * L + lo + n)
        new, fr = row_factor(r_old[rows, :], rows, level[2], D)
        s = jnp.zeros((n, L), F32)
        for j in range(NB_OUT):
            s = s + g2_out[lo:lo + n, j * L:(j + 1) * L] * fac[5, j:j + 1, :]
        usq = usq + jnp.sum(s * (fr * fr), axis=0, keepdims=True)
        row_sq[rows, :] = fr
        r_old[rows, :] = new
    m3[me, 2:3, :] = usq
    m3[me, 3:4, :] = jnp.zeros((1, L), F32)
    m3_out = bcast(m3, m3_send, m3_recv)

    for b, ref in enumerate((acc, grecv)):
        fr = row_sq[b * L:(b + 1) * L, :]
        for j in range(NB_IN):
            c = slice(j * L, (j + 1) * L)
            d_in[ks[b], :, c] = ref[0:XR, c] * fac[ks[b], j:j + 1, :] * fr
    for lo, n in ROWS_OUT:
        fr = row_sq[2 * L + lo:2 * L + lo + n, :]
        for j in range(NB_OUT):
            c = slice(j * L, (j + 1) * L)
            d_out[lo:lo + n, c] = d_out[lo:lo + n, c] * fac[2, j:j + 1, :] * fr
    for k in range(2):
        rin_new[k:k + 1, :] = r_old[k * L:(k + 1) * L, :].T[0:1, :]
        for j in range(NB_IN):
            cin_new[k:k + 1, j * L:(j + 1) * L] = c_old[k, j:j + 1, :]
    for lo in (0, L, 2 * L):
        rpad[:, lo:lo + L] = r_old[2 * L + lo:3 * L + lo, :].T[0:1, :]
    rout_new[...] = rpad[:, 0:HR].reshape(HR)
    for j in range(NB_OUT):
        cout_new[:, j * L:(j + 1) * L] = c_old[2, j:j + 1, :]

    exchange_wait(m4, m4_send, m4_recv)
    wsum = ((m4[0] + m4[1]) + (m4[2] + m4[3])) + ((m4[4] + m4[5]) + (m4[6] + m4[7]))
    wrms = jnp.sqrt(jnp.sum(wsum, axis=1, keepdims=True)[0:4, :] / (D * FF))
    step = rel[...] * jnp.maximum(EPS_TWO, wrms)
    exchange_wait(m3, m3_send, m3_recv)
    usum = ((m3[0] + m3[1]) + (m3[2] + m3[3])) + ((m3[4] + m3[5]) + (m3[6] + m3[7]))
    urms = jnp.sqrt(jnp.sum(usum, axis=1, keepdims=True) / (D * FF))
    kappa[0:4, :] = jnp.broadcast_to(step / jnp.maximum(1.0, urms / crms[...]), (4, L))
    kappa[4:8, :] = jnp.zeros((4, L), F32)

    for i in range(NC):
        x_send(i).wait_send()
    for p in range(HEAD):
        hid_send(p).wait_send()
    for cp in m1_out + m2_out + m3_out + m4_out:
        cp.wait_send()


def write_kernel(d_in, d_out, w_in, w_out, rin, cin, rout, cout, kappa,
                 wi_hbm, ri_hbm, ci_hbm, wo_hbm, ro_hbm, co_hbm, st_in, st_out, sem, sem_small):
    copies = []

    def put(src, dst, s):
        cp = pltpu.make_async_copy(src, dst, s)
        cp.start()
        copies.append(cp)

    n = len(copies)
    for lo, h in PARTS_OUT:
        r = slice(lo, lo + h)
        for j in range(NB_OUT):
            c = slice(j * L, (j + 1) * L)
            st_out[r, c] = w_out[r, c] - kappa[2:3, :] * d_out[r, c]
        put(st_out.at[pl.ds(lo, h)], wo_hbm.at[pl.ds(lo, h)], sem.at[n])
        n += 1
    for k in range(2):
        for lo in range(0, XR, XR // 4):
            h = XR // 4
            r = slice(lo, lo + h)
            for j in range(NB_IN):
                c = slice(j * L, (j + 1) * L)
                st_in[k, r, c] = w_in[k, r, c] - kappa[k:k + 1, :] * d_in[k, r, c]
            put(st_in.at[k, pl.ds(lo, h)], wi_hbm.at[k, pl.ds(lo, h)], sem.at[n])
            n += 1
        if k == 0:
            for m, (a, b) in enumerate(((rin, ri_hbm), (cin, ci_hbm), (rout, ro_hbm), (cout, co_hbm))):
                put(a, b, sem_small.at[m])
    for cp in copies:
        cp.wait()


def local_step(x_norm, hid_act, dy_in, dy_out, w_in, w_out, row_in, col_in, row_out, col_out,
               beta_two, rel_step, clip_rms, clip_norm):
    hbm = pl.BlockSpec(memory_space=pltpu.HBM)
    vmem = pl.BlockSpec(memory_space=pltpu.VMEM)
    dma = pltpu.SemaphoreType.DMA
    mids = [(2, XR, FF), (HR, D), (2, XR, FF), (HR, D), (2, XR), (2, FF), (HR,), (1, D), (8, L)]
    mid = pl.pallas_call(
        grad_kernel,
        out_shape=[pltpu.VMEM(s, F32) for s in mids],
        in_specs=[hbm] * 14,
        out_specs=[vmem] * len(mids),
        scratch_shapes=[
            pltpu.VMEM((T, XR), jnp.bfloat16), pltpu.VMEM((T, XR), jnp.bfloat16),
            pltpu.VMEM((2 * XR, KC), jnp.bfloat16), pltpu.VMEM((2 * XR, KC), jnp.bfloat16),
            pltpu.VMEM((HR, T), jnp.bfloat16), pltpu.VMEM((SLOTS, KC, FF), jnp.bfloat16),
            pltpu.VMEM((2 * XR, FF), F32), pltpu.VMEM((XR, FF), F32), pltpu.VMEM((2 * L, FF), F32), pltpu.VMEM((HR, D), F32),
            pltpu.VMEM((HR, D), F32), pltpu.VMEM((HR, D), F32),
            pltpu.VMEM((ND, 32, L), F32), pltpu.VMEM((ND, 8, L), F32), pltpu.VMEM((ND, 4, L), F32),
            pltpu.VMEM((ND, 8, L), F32), pltpu.VMEM((5 * L, L), F32), pltpu.VMEM((5 * L, L), F32),
            pltpu.VMEM((6, NP, L), F32), pltpu.VMEM((3, NP, L), F32), pltpu.VMEM((1, 3 * L), F32),
            pltpu.VMEM((2, XR), F32), pltpu.VMEM((2, FF), F32), pltpu.VMEM((HR,), F32), pltpu.VMEM((1, D), F32),
            pltpu.VMEM((1, 1), F32), pltpu.VMEM((1, 1), F32), pltpu.VMEM((1, 1), F32), pltpu.VMEM((1, 1), F32),
            dma((2,)), dma((PIECES,)), dma((PIECES,)), dma((NC,)), dma((2,)), dma((8,)), dma((NC,)), dma((NC,)),
            dma((HEAD,)), dma((HEAD,)), dma((2,)),
            dma(()), dma(()), dma((ND,)), dma((ND,)), dma((ND,)), dma((ND,)), dma((ND,)), dma((ND,)), dma((ND,)),
            dma((ND,)),
        ],
        compiler_params=pltpu.CompilerParams(collective_id=0, has_side_effects=True, vmem_limit_bytes=52 << 20),
        name="grad_stats",
    )(x_norm, hid_act.T, dy_in, dy_out, w_in, w_out, row_in, col_in,
      row_out, col_out.reshape(1, D),
      beta_two.reshape(1, 1), rel_step.reshape(1, 1), clip_rms.reshape(1, 1), clip_norm.reshape(1, 1))
    mid = [pltpu.with_memory_space_constraint(v, pltpu.VMEM) for v in mid]
    outs = [(2, XR, FF), (2, XR), (2, FF), (HR, D), (HR,), (1, D)]
    out = pl.pallas_call(
        write_kernel,
        out_shape=[pltpu.HBM(s, F32) for s in outs],
        in_specs=[vmem] * len(mids),
        out_specs=[hbm] * len(outs),
        scratch_shapes=[pltpu.VMEM((2, XR, FF), F32), pltpu.VMEM((HR, D), F32), dma((12,)), dma((4,))],
        compiler_params=pltpu.CompilerParams(vmem_limit_bytes=12 << 20),
        name="write_weights",
    )(*mid)
    return (out[0], out[1], out[2], out[3], out[4], out[5].reshape(D))


def solution(mesh):
    in_specs = (P(None, 'tp'), P(None, 'tp'), P(), P(), P(None, 'tp', None), P('tp', None),
                P(None, 'tp'), P(), P('tp'), P(), P(), P(), P(), P())
    out_specs = (P(None, 'tp', None), P(None, 'tp'), P(), P('tp', None), P('tp'), P())
    return jax.shard_map(local_step, mesh=mesh, in_specs=in_specs, out_specs=out_specs, check_vma=False)
```

```python
import jax
import jax.numpy as jnp
from jax import lax
from jax.experimental import pallas as pl
from jax.experimental.pallas import tpu as pltpu
from jax.sharding import PartitionSpec as P

EPS_ONE = 1e-30
EPS_TWO = 1e-3
MESH = pl.DeviceIdType.MESH
F32 = jnp.float32

T = 8192
D = 1024
FF = 2816
ND = 8
XR = D // ND
HR = FF // ND
KC = 1024
NC = T // KC
L = 128
NB_IN = FF // L
NB_OUT = D // L
NP = 24
ROWS_OUT = ((0, L), (L, L), (2 * L, HR - 2 * L))
TILE = 2 * L
SLOTS = 4
PARTS_OUT = ((0, 32), (32, 64), (96, L), (224, L))
HEAD = 2
PIECES = NC - HEAD


def total(v):
    return jnp.sum(jnp.sum(v, axis=0, keepdims=True), axis=1, keepdims=True)


def spread(row):
    return jnp.broadcast_to(row, (L, row.shape[1])).T


def grad_kernel(x_hbm, hid_hbm, dyi_hbm, dyo_hbm, wi_hbm, wo_hbm, ri_hbm, ci_hbm, ro_hbm, co_hbm,
                beta_hbm, rel_hbm, crms_hbm, cnorm_hbm,
                d_in, d_out, w_in, w_out, rin_new, cin_new, rout_new, cout_new, kappa,
                x_own, x_peer, xt0, xt1, hid, ring, acc, grecv, go_send, go_recv, m1, m2, m3, m4, row_sq, r_old, fac, c_old, rpad,
                ri, ci, ro, co, beta, rel, crms, cnorm,
                s_x, s_hid, s_dyo, s_dyi, s_w, s_small, xs_send, xs_recv, hs_send, hs_recv, go_sems, g_send, g_recv,
                m1_send, m1_recv, m2_send, m2_recv, m3_send, m3_recv, m4_send, m4_recv):
    me = lax.axis_index("tp")
    chip = me // 2
    core = me - 2 * chip
    other = 1 - core
    peer = 2 * chip + other
    diag = 3 - chip
    xn = chip + 1 - 2 * lax.rem(chip, 2)
    yn = lax.rem(chip + 2, 4)
    others = [2 * diag + core, 2 * diag + other, 2 * xn + core, 2 * yn + core, 2 * xn + other, 2 * yn + other, peer]

    def token(p, who):
        return pl.multiple_of((who * HEAD + p) * KC, KC) if p < HEAD else (p + HEAD) * KC

    def kept(p):
        return p * KC if p < HEAD else (p + HEAD) * KC

    def out_copies(p):
        rows = pl.ds(token(p, core), KC)
        return (pltpu.make_async_copy(hid_hbm.at[:, rows], hid.at[:, pl.ds(kept(p), KC)], s_hid.at[p]),
                pltpu.make_async_copy(dyo_hbm.at[rows, :], ring.at[p // 2, :, pl.ds(p % 2 * D, D)], s_dyo.at[p]))

    def hid_send(p):
        return pltpu.make_async_remote_copy(hid_hbm.at[:, pl.ds(token(p, other), KC)],
                                            hid.at[:, pl.ds((HEAD + p) * KC, KC)], hs_send.at[p], hs_recv.at[p],
                                            device_id=(peer,), device_id_type=MESH)

    def start_out(*ps):
        for p in ps:
            for cp in out_copies(p):
                cp.start()

    def dyi_copy(i):
        return pltpu.make_async_copy(dyi_hbm.at[core, pl.ds(i * KC, KC), :], ring.at[(i + 1) % SLOTS], s_dyi.at[i])

    def x_send(i):
        c = pl.ds(i * KC, KC)
        return pltpu.make_async_remote_copy(x_own.at[c, :], x_peer.at[c, :], xs_send.at[i], xs_recv.at[i],
                                            device_id=(peer,), device_id_type=MESH)

    def bcast(buf, send, recv):
        out = [pltpu.make_async_remote_copy(buf.at[me], buf.at[me], send.at[k], recv.at[me],
                                            device_id=(dst,), device_id_type=MESH) for k, dst in enumerate(others)]
        for cp in out:
            cp.start()
        return out

    def exchange_wait(buf, send, recv):
        for k, src in reversed(list(enumerate(others))):
            pltpu.make_async_remote_copy(buf.at[src], buf.at[src], send.at[k], recv.at[src],
                                         device_id=(src,), device_id_type=MESH).wait_recv()

    x_loads = [pltpu.make_async_copy(x_hbm.at[r, :], x_own.at[r, :], s_x.at[n])
               for n, r in enumerate((pl.ds(0, KC), pl.ds(KC, T - KC)))]
    start_out(0)
    x_loads[0].start()
    start_out(1)
    dyi_copy(0).start()
    x_loads[1].start()
    dyi_copy(1).start()
    small = [pltpu.make_async_copy(a, b, s_small.at[n]) for n, (a, b) in enumerate(
        ((ri_hbm, ri), (ci_hbm, ci), (ro_hbm, ro), (co_hbm, co),
         (beta_hbm, beta), (rel_hbm, rel), (crms_hbm, crms), (cnorm_hbm, cnorm)))]
    for cp in small:
        cp.start()

    barrier = pltpu.get_barrier_semaphore()
    for dst in others:
        pl.semaphore_signal(barrier, inc=1, device_id=(dst,), device_id_type=MESH)
    rpad[...] = jnp.zeros_like(rpad)

    def wait_out(p):
        for cp in out_copies(p):
            cp.wait()

    def out_step(p, *extra):
        for n in range(D // TILE):
            c = pl.ds(n * TILE, TILE)
            v = jnp.dot(hid[:, pl.ds(kept(p), KC)], ring[p // 2, :, pl.ds(p % 2 * D + n * TILE, TILE)],
                        preferred_element_type=F32)
            if p == HEAD:
                v = v + go_recv[:, c]
            d_out[:, c] = v if p == 0 else d_out[:, c] + v
            if n < len(extra):
                extra[n]()

    def partner_step(p, turn=False):
        for n in range(D // TILE):
            c = pl.ds(n * TILE, TILE)
            v = jnp.dot(hid[:, pl.ds((HEAD + p) * KC, KC)], ring[0, :, pl.ds(p * D + n * TILE, TILE)],
                        preferred_element_type=F32)
            go_send[:, c] = v if p == 0 else go_send[:, c] + v
            if turn:
                transpose(1, n)

    xt = (xt0, xt1)
    QT = KC // 4

    def transpose(i, n):
        rows = pl.ds(i * KC + n * QT, QT)
        cols = slice(n * QT, (n + 1) * QT)
        xt[i % 2][0:XR, cols] = x_own[rows, :].T
        xt[i % 2][XR:2 * XR, cols] = x_peer[rows, :].T

    own, both = slice(0, XR), slice(0, 2 * XR)
    blocks = [(both, n * TILE) for n in range(FF // TILE - 1)] + [(own, FF - TILE), (slice(XR, 2 * XR), FF - TILE)]

    def in_step(i):
        for n, (rows, c0) in enumerate(blocks):
            c = slice(c0, c0 + TILE)
            v = jnp.dot(xt[i % 2][rows, :], ring[(i + 1) % SLOTS, :, c], preferred_element_type=F32)
            acc[rows, c] = v if i == 0 else acc[rows, c] + v
            if n < 4 and 0 < i < NC - 1:
                transpose(i + 1, n)

    go_copy = pltpu.make_async_remote_copy(go_send, go_recv, go_sems.at[0], go_sems.at[1],
                                           device_id=(peer,), device_id_type=MESH)
    pl.semaphore_wait(barrier, ND - 1)
    x_loads[0].wait()
    x_send(0).start()
    wait_out(0)
    out_step(0)
    dyi_copy(2).start()
    for p in range(HEAD):
        hid_send(p).start()
    wait_out(1)
    out_step(1)
    x_send(0).wait_recv()
    for n in range(4):
        transpose(0, n)
    for i in range(NC):
        if 0 < i < NC - 1:
            x_send(i + 1).wait_recv()
        dyi_copy(i).wait()
        in_step(i)
        if i == 0:
            x_loads[1].wait()
            for k in range(1, NC):
                x_send(k).start()
            hid_send(0).wait_recv()
            partner_step(0)
            hid_send(1).wait_recv()
            x_send(1).wait_recv()
            partner_step(1, True)
            dyi_copy(3).start()
        if i == 1:
            go_copy.start()
        if i in (1, 3):
            dyi_copy(i + 3).start()
            dyi_copy(i + 4).start()
        if i == NC - 3:
            start_out(2, 3, 4, 5)

    loads = [pltpu.make_async_copy(wi_hbm, w_in, s_w.at[0]), pltpu.make_async_copy(wo_hbm, w_out, s_w.at[1])]
    for cp in loads:
        cp.start()

    def stats_early():
        for j in range(NB_IN):
            g = acc[:, j * L:(j + 1) * L]
            m1[me, j:j + 1, :] = jnp.sum(g * g, axis=0, keepdims=True)
        rpad[:, 0:HR] = ro[...].reshape(1, HR)
        m1[me, NB_IN:NP, :] = jnp.zeros((NP - NB_IN, L), F32)
        m1[me, NP:26, :] = ri[...]
        m1[me, 26:27, :] = rpad[:, 0:L] + rpad[:, L:2 * L] + rpad[:, 2 * L:3 * L]
        m1[me, 27:32, :] = jnp.zeros((5, L), F32)

    for cp in small:
        cp.wait()
    wait_out(2)
    go_copy.wait()
    g_copy = pltpu.make_async_remote_copy(acc.at[pl.ds(XR, XR), :], grecv, g_send, g_recv,
                                          device_id=(peer,), device_id_type=MESH)
    g_copy.start()
    out_step(2, stats_early)
    m1_out = bcast(m1, m1_send, m1_recv)

    def stats_own(b, ref):
        def body():
            s = jnp.zeros((XR, L), F32)
            for j in range(NB_IN):
                c = slice(j * L, (j + 1) * L)
                g = ref[0:XR, c]
                s = s + g * g
            row_sq[b * L:(b + 1) * L, :] = jnp.broadcast_to(jnp.sum(s, axis=1, keepdims=True), (XR, L))
        return body

    def old_stats():
        for k in range(2):
            r_old[k * L:(k + 1) * L, :] = spread(ri[k:k + 1, :])
            for j in range(NB_IN):
                c_old[k, j:j + 1, :] = ci[k:k + 1, j * L:(j + 1) * L]
            c_old[k, NB_IN:NP, :] = jnp.ones((NP - NB_IN, L), F32)
        for lo in (0, L, 2 * L):
            r_old[2 * L + lo:3 * L + lo, :] = spread(rpad[:, lo:lo + L])
        for j in range(NB_OUT):
            c_old[2, j:j + 1, :] = co[:, j * L:(j + 1) * L]

    wait_out(3)
    out_step(3, stats_own(0, acc))
    wait_out(4)
    out_step(4, old_stats)
    wait_out(5)
    out_step(5)

    for j in range(NB_OUT):
        g = d_out[:, j * L:(j + 1) * L]
        m2[me, j:j + 1, :] = jnp.sum(g * g, axis=0, keepdims=True)
    m2_out = bcast(m2, m2_send, m2_recv)

    for lo, n in ROWS_OUT:
        s = jnp.zeros((n, L), F32)
        for j in range(NB_OUT):
            c = slice(j * L, (j + 1) * L)
            g = d_out[lo:lo + n, c]
            s = s + g * g
        row_sq[2 * L + lo:2 * L + lo + n, :] = jnp.broadcast_to(jnp.sum(s, axis=1, keepdims=True), (n, L))
    g_copy.wait()
    stats_own(1, grecv)()
    for cp in loads:
        cp.wait()
    m4[me] = jnp.zeros((8, L), F32)
    for k in range(2):
        w_sq = jnp.zeros((8, L), F32)
        for j in range(NB_IN):
            w = w_in[k, :, j * L:(j + 1) * L]
            w_sq = w_sq + jnp.sum((w * w).reshape(XR // 8, 8, L), axis=0)
        m4[me, k:k + 1, :] = jnp.sum(w_sq, axis=0, keepdims=True)
    w_sq = jnp.zeros((8, L), F32)
    for j in range(NB_OUT):
        w = w_out[:, j * L:(j + 1) * L]
        w_sq = w_sq + jnp.sum((w * w).reshape(HR // 8, 8, L), axis=0)
    m4[me, 2:3, :] = jnp.sum(w_sq, axis=0, keepdims=True)
    m4_out = bcast(m4, m4_send, m4_recv)

    exchange_wait(m1, m1_send, m1_recv)
    b2 = beta[...]
    mix = 1.0 - b2
    col = [(m1[0, 0:NP] + m1[2, 0:NP]) + (m1[4, 0:NP] + m1[6, 0:NP]),
           (m1[1, 0:NP] + m1[3, 0:NP]) + (m1[5, 0:NP] + m1[7, 0:NP])]
    tail = slice(NP, 32)
    scal = ((m1[0, tail] + m1[1, tail]) + (m1[2, tail] + m1[3, tail])) + (
        (m1[4, tail] + m1[5, tail]) + (m1[6, tail] + m1[7, tail]))
    scal = jnp.sum(scal, axis=1, keepdims=True)
    tot = [total(v) for v in col]
    exchange_wait(m2, m2_send, m2_recv)
    col.append(((m2[0] + m2[1]) + (m2[2] + m2[3])) + ((m2[4] + m2[5]) + (m2[6] + m2[7])))
    tot.append(total(col[2]))
    norm_sq = tot[0] + tot[1] + tot[2]
    gs = jnp.minimum(1.0, cnorm[...] / jnp.sqrt(norm_sq))

    shape = [(D, FF), (D, FF), (FF, D)]
    level = [b2 * scal[k:k + 1, :] / m + mix * (gs * (gs * tot[k]) / (m * n) + EPS_ONE)
             for k, (m, n) in enumerate(shape)]

    for k in range(3):
        nb = NP if k < 2 else NB_OUT
        new = b2 * c_old[k, 0:nb] + mix * (gs * (gs * col[k]) / shape[k][0] + EPS_ONE)
        c_old[k, 0:nb] = new
        fac[k, 0:nb] = gs * lax.rsqrt(new)

    def row_factor(old, rows, lvl, n):
        new = b2 * old + mix * (gs * (gs * row_sq[rows, :]) / n + EPS_ONE)
        return new, lax.rsqrt(new / lvl)

    is0 = core == 0
    ks = (core, other)
    for b, ref in enumerate((acc, grecv)):
        rows = slice(b * L, (b + 1) * L)
        lvl = jnp.where(is0 if b == 0 else jnp.logical_not(is0), level[0], level[1])
        new, fr = row_factor(r_old[pl.ds(pl.multiple_of(ks[b] * L, L), L), :], rows, lvl, FF)
        s = jnp.zeros((XR, L), F32)
        for j in range(NB_IN):
            v = ref[0:XR, j * L:(j + 1) * L] * fac[ks[b], j:j + 1, :]
            s = s + v * v
        m3[me, pl.ds(ks[b], 1), :] = jnp.sum(s * (fr * fr), axis=0, keepdims=True)
        row_sq[rows, :] = fr
        r_old[pl.ds(pl.multiple_of(ks[b] * L, L), L), :] = new
    usq = jnp.zeros((1, L), F32)
    for lo, n in ROWS_OUT:
        rows = slice(2 * L + lo, 2 * L + lo + n)
        new, fr = row_factor(r_old[rows, :], rows, level[2], D)
        s = jnp.zeros((n, L), F32)
        for j in range(NB_OUT):
            v = d_out[lo:lo + n, j * L:(j + 1) * L] * fac[2, j:j + 1, :]
            s = s + v * v
        usq = usq + jnp.sum(s * (fr * fr), axis=0, keepdims=True)
        row_sq[rows, :] = fr
        r_old[rows, :] = new
    m3[me, 2:3, :] = usq
    m3[me, 3:4, :] = jnp.zeros((1, L), F32)
    m3_out = bcast(m3, m3_send, m3_recv)

    for b, ref in enumerate((acc, grecv)):
        fr = row_sq[b * L:(b + 1) * L, :]
        for j in range(NB_IN):
            c = slice(j * L, (j + 1) * L)
            d_in[ks[b], :, c] = ref[0:XR, c] * fac[ks[b], j:j + 1, :] * fr
    for lo, n in ROWS_OUT:
        fr = row_sq[2 * L + lo:2 * L + lo + n, :]
        for j in range(NB_OUT):
            c = slice(j * L, (j + 1) * L)
            d_out[lo:lo + n, c] = d_out[lo:lo + n, c] * fac[2, j:j + 1, :] * fr
    for k in range(2):
        rin_new[k:k + 1, :] = r_old[k * L:(k + 1) * L, :].T[0:1, :]
        for j in range(NB_IN):
            cin_new[k:k + 1, j * L:(j + 1) * L] = c_old[k, j:j + 1, :]
    for lo in (0, L, 2 * L):
        rpad[:, lo:lo + L] = r_old[2 * L + lo:3 * L + lo, :].T[0:1, :]
    rout_new[...] = rpad[:, 0:HR].reshape(HR)
    for j in range(NB_OUT):
        cout_new[:, j * L:(j + 1) * L] = c_old[2, j:j + 1, :]

    exchange_wait(m4, m4_send, m4_recv)
    wsum = ((m4[0] + m4[1]) + (m4[2] + m4[3])) + ((m4[4] + m4[5]) + (m4[6] + m4[7]))
    wrms = jnp.sqrt(jnp.sum(wsum, axis=1, keepdims=True)[0:4, :] / (D * FF))
    step = rel[...] * jnp.maximum(EPS_TWO, wrms)
    exchange_wait(m3, m3_send, m3_recv)
    usum = ((m3[0] + m3[1]) + (m3[2] + m3[3])) + ((m3[4] + m3[5]) + (m3[6] + m3[7]))
    urms = jnp.sqrt(jnp.sum(usum, axis=1, keepdims=True) / (D * FF))
    kappa[0:4, :] = jnp.broadcast_to(step / jnp.maximum(1.0, urms / crms[...]), (4, L))
    kappa[4:8, :] = jnp.zeros((4, L), F32)

    for i in range(NC):
        x_send(i).wait_send()
    for p in range(HEAD):
        hid_send(p).wait_send()
    for cp in m1_out + m2_out + m3_out + m4_out:
        cp.wait_send()


def write_kernel(d_in, d_out, w_in, w_out, rin, cin, rout, cout, kappa,
                 wi_hbm, ri_hbm, ci_hbm, wo_hbm, ro_hbm, co_hbm, st_in, st_out, sem, sem_small):
    copies = []

    def put(src, dst, s):
        cp = pltpu.make_async_copy(src, dst, s)
        cp.start()
        copies.append(cp)

    n = len(copies)
    for lo, h in PARTS_OUT:
        r = slice(lo, lo + h)
        for j in range(NB_OUT):
            c = slice(j * L, (j + 1) * L)
            st_out[r, c] = w_out[r, c] - kappa[2:3, :] * d_out[r, c]
        put(st_out.at[pl.ds(lo, h)], wo_hbm.at[pl.ds(lo, h)], sem.at[n])
        n += 1
    for k in range(2):
        for lo in range(0, XR, XR // 4):
            h = XR // 4
            r = slice(lo, lo + h)
            for j in range(NB_IN):
                c = slice(j * L, (j + 1) * L)
                st_in[k, r, c] = w_in[k, r, c] - kappa[k:k + 1, :] * d_in[k, r, c]
            put(st_in.at[k, pl.ds(lo, h)], wi_hbm.at[k, pl.ds(lo, h)], sem.at[n])
            n += 1
        if k == 0:
            for m, (a, b) in enumerate(((rin, ri_hbm), (cin, ci_hbm), (rout, ro_hbm), (cout, co_hbm))):
                put(a, b, sem_small.at[m])
    for cp in copies:
        cp.wait()


def local_step(x_norm, hid_act, dy_in, dy_out, w_in, w_out, row_in, col_in, row_out, col_out,
               beta_two, rel_step, clip_rms, clip_norm):
    hbm = pl.BlockSpec(memory_space=pltpu.HBM)
    vmem = pl.BlockSpec(memory_space=pltpu.VMEM)
    dma = pltpu.SemaphoreType.DMA
    mids = [(2, XR, FF), (HR, D), (2, XR, FF), (HR, D), (2, XR), (2, FF), (HR,), (1, D), (8, L)]
    mid = pl.pallas_call(
        grad_kernel,
        out_shape=[pltpu.VMEM(s, F32) for s in mids],
        in_specs=[hbm] * 14,
        out_specs=[vmem] * len(mids),
        scratch_shapes=[
            pltpu.VMEM((T, XR), jnp.bfloat16), pltpu.VMEM((T, XR), jnp.bfloat16),
            pltpu.VMEM((2 * XR, KC), jnp.bfloat16), pltpu.VMEM((2 * XR, KC), jnp.bfloat16),
            pltpu.VMEM((HR, T), jnp.bfloat16), pltpu.VMEM((SLOTS, KC, FF), jnp.bfloat16),
            pltpu.VMEM((2 * XR, FF), F32), pltpu.VMEM((XR, FF), F32),
            pltpu.VMEM((HR, D), F32), pltpu.VMEM((HR, D), F32),
            pltpu.VMEM((ND, 32, L), F32), pltpu.VMEM((ND, 8, L), F32), pltpu.VMEM((ND, 4, L), F32),
            pltpu.VMEM((ND, 8, L), F32), pltpu.VMEM((5 * L, L), F32), pltpu.VMEM((5 * L, L), F32),
            pltpu.VMEM((3, NP, L), F32), pltpu.VMEM((3, NP, L), F32), pltpu.VMEM((1, 3 * L), F32),
            pltpu.VMEM((2, XR), F32), pltpu.VMEM((2, FF), F32), pltpu.VMEM((HR,), F32), pltpu.VMEM((1, D), F32),
            pltpu.VMEM((1, 1), F32), pltpu.VMEM((1, 1), F32), pltpu.VMEM((1, 1), F32), pltpu.VMEM((1, 1), F32),
            dma((2,)), dma((PIECES,)), dma((PIECES,)), dma((NC,)), dma((2,)), dma((8,)), dma((NC,)), dma((NC,)),
            dma((HEAD,)), dma((HEAD,)), dma((2,)),
            dma(()), dma(()), dma((ND,)), dma((ND,)), dma((ND,)), dma((ND,)), dma((ND,)), dma((ND,)), dma((ND,)),
            dma((ND,)),
        ],
        compiler_params=pltpu.CompilerParams(collective_id=0, has_side_effects=True, vmem_limit_bytes=52 << 20),
        name="grad_stats",
    )(x_norm, hid_act.T, dy_in, dy_out, w_in, w_out, row_in, col_in,
      row_out, col_out.reshape(1, D),
      beta_two.reshape(1, 1), rel_step.reshape(1, 1), clip_rms.reshape(1, 1), clip_norm.reshape(1, 1))
    mid = [pltpu.with_memory_space_constraint(v, pltpu.VMEM) for v in mid]
    outs = [(2, XR, FF), (2, XR), (2, FF), (HR, D), (HR,), (1, D)]
    out = pl.pallas_call(
        write_kernel,
        out_shape=[pltpu.HBM(s, F32) for s in outs],
        in_specs=[vmem] * len(mids),
        out_specs=[hbm] * len(outs),
        scratch_shapes=[pltpu.VMEM((2, XR, FF), F32), pltpu.VMEM((HR, D), F32), dma((12,)), dma((4,))],
        compiler_params=pltpu.CompilerParams(vmem_limit_bytes=12 << 20),
        name="write_weights",
    )(*mid)
    return (out[0], out[1], out[2], out[3], out[4], out[5].reshape(D))


def solution(mesh):
    in_specs = (P(None, 'tp'), P(None, 'tp'), P(), P(), P(None, 'tp', None), P('tp', None),
                P(None, 'tp'), P(), P('tp'), P(), P(), P(), P(), P())
    out_specs = (P(None, 'tp', None), P(None, 'tp'), P(), P('tp', None), P('tp'), P())
    return jax.shard_map(local_step, mesh=mesh, in_specs=in_specs, out_specs=out_specs, check_vma=False)
```
